32 devices in a mesh: atm: 4 (over z), land: 8 (over y, x, core).
Axes of the slice: x: 2, y: 2, z: 4, core: 2. Of those that a mesh axis runs over, the one named last changes fastest.
Arguments:
- tile_forcing: bfloat16 [4096, 128], P(('atm', 'land')), may hold values from -6 to 6
- elevation_gap: float32 [65536], P(('atm', 'land')), may hold values from -5 to 5
- lapse_rate: float32 [128], replicated, may hold values from -3 to 3
- column_tile: int32 [65536], P(('atm', 'land')), may hold values from 0 to 127
- column_target: int32 [65536], P(('atm', 'land')), may hold values from 0 to 163839, as said below
- owner_counts: int32 [32], P(('atm', 'land')), may hold values from 1 to 5120, as said below
- land_state: float32 [163840, 128], P(('atm', 'land')), may hold values from -6 to 6
- w_in: bfloat16 [256, 1024], replicated, may hold values from -0.375 to 0.375
- norm_gains: float32 [2, 1024], replicated, may hold values from 0.5 to 1.5
- w_up: bfloat16 [1, 1024, 1024], replicated, may hold values from -0.1875 to 0.1875
- w_down: bfloat16 [1, 1024, 1024], replicated, may hold values from -0.1875 to 0.1875
- w_out: bfloat16 [1024, 256], replicated, may hold values from -0.1875 to 0.1875
Outputs:
- new_state: float32 [163840, 128], P(('atm', 'land'))
- tile_flux: float32 [4096, 128], P(('atm', 'land'))
The draws below stay inside these ranges and needn't reach their ends.
Inputs may be any that keep to these rules, and one draw needn't show every extreme that they name: `column_target`: live slots of owner j are j * 5120 to j * 5120 + owner_counts[j] - 1; every live slot is named by exactly one column and no other slot is named. The columns of one device name at most 161 slots of any one owner, and some pair reaches 161. `owner_counts`: they sum to 65536; the largest is exactly 5120. `column_tile`: index of the column's tile among the 128 tiles of the device that holds the column.
All inputs are finite; a program needn't handle non-finite values.
Results may differ from the reference program's by a relative error of at most 0.0038.
Values may be sent and summed in bfloat16 or wider, within the bound.
No kernel may reach another device: no remote copies, remote signals or barrier semaphores. Data moves between devices by JAX's collectives and lax.ppermute only.
A program may use at most 128 MiB of HBM per device.

```python
import jax
import jax.numpy as jnp
from jax import lax

FORCING = 128
STATE = 128
FLUX = 128
HIDDEN_SIZE = 1024
LAYERS = 1
A_COLS = 2048
TILE_DEV = 128
FEATURES = 256
CAP = 5120
COLS = 65536
SLOTS = 163840
TILES = 4096


def routing_tables(key):
    base = jax.random.fold_in(key, 7321)
    owners = COLS // A_COLS
    middle = A_COLS // owners
    most = 5 * middle // 2
    busy = owners // 8
    order = jax.random.permutation(jax.random.fold_in(base, 1), owners)
    placing = jnp.zeros((owners,), jnp.int32).at[order].set(jnp.arange(owners, dtype=jnp.int32))
    is_busy = placing < busy
    others = owners - busy
    extra = busy * (most - middle)
    lowered = extra // others + (placing - busy < extra % others).astype(jnp.int32)
    share = jnp.where(is_busy, most, middle - lowered).astype(jnp.int32)
    bump = jnp.where(is_busy, 1, jnp.where((placing >= busy) & (placing < 2 * busy), -1, 0)).astype(jnp.int32)
    sender_order = jax.random.permutation(jax.random.fold_in(base, 2), owners)
    signs = jnp.where(sender_order < owners // 2, 1, -1).astype(jnp.int32)
    load = share[None, :] + signs[:, None] * bump[None, :]
    offsets = jnp.cumsum(load, axis=0) - load
    ends = jnp.cumsum(load, axis=1)
    starts = ends - load

    def one_sender(sender):
        position = jnp.arange(A_COLS, dtype=jnp.int32)
        receiver = jnp.sum((ends[sender][None, :] <= position[:, None]).astype(jnp.int32), axis=1)
        within = position - starts[sender][receiver]
        target = receiver * CAP + offsets[sender][receiver] + within
        shuffle = jax.random.permutation(jax.random.fold_in(jax.random.fold_in(base, 3), sender), A_COLS)
        return target[shuffle].astype(jnp.int32)
    targets = lax.map(one_sender, jnp.arange(owners, dtype=jnp.int32))
    return (targets.reshape(COLS), (owners * share).astype(jnp.int32))


def draw_column_target(key, part):
    return routing_tables(key)[0]


def draw_owner_counts(key, part):
    return routing_tables(key)[1]


def touch_ends(entries, rng, smallest, top_value):
    place = [jax.random.randint(jax.random.fold_in(rng, axis), (), 0, length) for axis, length in enumerate(entries.shape)]
    longest = entries.shape.index(max(entries.shape))
    neighbour = place[:longest] + [(place[longest] + 1) % entries.shape[longest]] + place[longest + 1:]
    return entries.at[tuple(place)].set(smallest).at[tuple(neighbour)].set(top_value)


def steps_of(stream_key, dims, split, least, largest):
    loudness, own = 1.0, jax.random.fold_in(stream_key, 6)
    for dim, shards_of in split:
        draws = jnp.exp(jax.random.uniform(jax.random.fold_in(own, dim), (shards_of,), jnp.float32, least / len(split), largest / len(split)))
        loudness = loudness * jnp.repeat(draws, dims[dim] // shards_of).reshape([-1 if axis == dim else 1 for axis in range(len(dims))])
    return loudness


def noise(own_key, extent, spread, reach, pieces=(), kind=jnp.bfloat16):
    loudness = steps_of(own_key, extent, pieces, -0.22, 0.18) if pieces else 1.0
    entries = jax.random.normal(own_key, extent, jnp.float32) * spread * loudness
    return jnp.minimum(jnp.maximum(entries, -reach), reach).astype(kind)


def setup_inputs(seed: int = 0) -> dict:
    seeds = jax.random.split(jax.random.key(seed), 13)
    return {
        "tile_forcing": noise(seeds[0], (TILES, FORCING), 1.0, 6.0, ((0, 32),)),
        "elevation_gap": noise(seeds[1], (COLS,), 1.0, 5.0, ((0, 32),), jnp.float32),
        "lapse_rate": noise(seeds[2], (FORCING,), 0.6, 3.0, (), jnp.float32),
        "column_tile": touch_ends(jax.random.randint(seeds[3], (COLS,), 0, TILE_DEV), jax.random.fold_in(seeds[3], 1), 0, TILE_DEV - 1).astype(jnp.int32),
        "column_target": draw_column_target(jax.random.fold_in(seeds[12], 71), 0),
        "owner_counts": draw_owner_counts(jax.random.fold_in(seeds[12], 71), 0),
        "land_state": noise(seeds[6], (SLOTS, STATE), 1.0, 6.0, ((0, 32),), jnp.float32),
        "w_in": noise(seeds[7], (FEATURES, HIDDEN_SIZE), FEATURES ** -0.5, 0.375),
        "norm_gains": jnp.clip(1.0 + 0.1 * jax.random.normal(seeds[8], (LAYERS + 1, HIDDEN_SIZE), jnp.float32), 0.5, 1.5),
        "w_up": noise(seeds[9], (LAYERS, HIDDEN_SIZE, HIDDEN_SIZE), HIDDEN_SIZE ** -0.5, 0.1875),
        "w_down": noise(seeds[10], (LAYERS, HIDDEN_SIZE, HIDDEN_SIZE), HIDDEN_SIZE ** -0.5, 0.1875),
        "w_out": noise(seeds[11], (HIDDEN_SIZE, STATE + FLUX), HIDDEN_SIZE ** -0.5, 0.1875),
    }


def normed(hidden, gain):
    scale = lax.rsqrt(lax.optimization_barrier(jnp.mean(hidden * hidden, axis=-1, keepdims=True)) + 1e-06)
    return hidden * scale * gain

def network(inputs, w_in, norm_gains, w_up, w_down, w_out):
    hidden = jnp.dot(inputs, w_in, preferred_element_type=jnp.float32)
    for layer in range(w_up.shape[0]):
        lowered = normed(hidden, norm_gains[layer]).astype(jnp.bfloat16)
        active = jax.nn.silu(jnp.dot(lowered, w_up[layer], preferred_element_type=jnp.float32)).astype(jnp.bfloat16)
        hidden = hidden + jnp.dot(active, w_down[layer], preferred_element_type=jnp.float32)
    lowered = normed(hidden, norm_gains[w_up.shape[0]]).astype(jnp.bfloat16)
    return jnp.dot(lowered, w_out, preferred_element_type=jnp.float32).astype(jnp.bfloat16)

def reference(tile_forcing, elevation_gap, lapse_rate, column_tile, column_target, owner_counts, land_state, w_in, norm_gains, w_up, w_down, w_out):
    column_index = jnp.arange(COLS, dtype=jnp.int32)
    tile_of = (column_tile + column_index // A_COLS * TILE_DEV).astype(jnp.int32)
    column_forcing = (tile_forcing.astype(jnp.float32)[tile_of] + elevation_gap[:, None] * lapse_rate[None, :]).astype(jnp.bfloat16)
    state_in = land_state.astype(jnp.bfloat16)
    inputs = jnp.concatenate([column_forcing, state_in[column_target]], axis=1)
    blocks = inputs.reshape(COLS // A_COLS, A_COLS, FEATURES)
    result = lax.map(lambda block: network(block, w_in, norm_gains, w_up, w_down, w_out), blocks)
    result = result.reshape(COLS, STATE + FLUX)
    tendency = jnp.zeros((SLOTS, STATE), jnp.float32).at[column_target].set(result[:, :STATE].astype(jnp.float32))
    slot_index = jnp.arange(SLOTS, dtype=jnp.int32)
    living = slot_index % CAP < owner_counts[slot_index // CAP]
    new_state = jnp.where(living[:, None], land_state + tendency, jnp.float32(0.0))
    flux = result[:, STATE:].astype(jnp.float32)
    totals = jax.ops.segment_sum(flux, tile_of, TILES)
    numbers = jax.ops.segment_sum(jnp.ones((COLS,), jnp.float32), tile_of, TILES)
    tile_flux = totals / jnp.maximum(numbers, 1.0)[:, None]
    return (new_state, tile_flux)
```

```python
import functools

import jax
import jax.numpy as jnp
from jax import lax
from jax.experimental import pallas as pl
from jax.experimental.pallas import tpu as pltpu
from jax.sharding import PartitionSpec as P

AXES = ("atm", "land")
ROWS = 256
FIELDS = 8
VMEM = pl.BlockSpec(memory_space=pltpu.VMEM)
SMEM = pl.BlockSpec(memory_space=pltpu.SMEM)
BF16 = jnp.bfloat16
F32 = jnp.float32


def iota(shape, dim):
    return lax.broadcasted_iota(jnp.int32, shape, dim)


def dot_nt(a, b):
    return lax.dot_general(a, b, (((1,), (1,)), ((), ())), preferred_element_type=F32)


def bucket_kernel(devices, capacity, tgt_ref, tile_ref, gap_ref, out_ref, count_ref):
    columns = tgt_ref.shape[1]
    places = out_ref.shape[1]
    tiles = count_ref.shape[0]
    target = tgt_ref[...]
    peer = jnp.floor((target.astype(F32) + 0.5) * (1.0 / capacity)).astype(jnp.int32)
    slot = target - peer * capacity
    high, low = lax.shift_right_logical(slot, 8), slot & (ROWS - 1)
    tile = tile_ref[...]
    gap = gap_ref[...]
    gap1 = gap.astype(BF16).astype(F32)
    gap2 = (gap - gap1).astype(BF16).astype(F32)
    gap3 = gap - gap1 - gap2
    hot = iota((devices, columns), 0) == peer
    hot_f = jnp.where(hot, 1.0, 0.0)
    hot_b = hot_f.astype(BF16)
    block = min(256, columns)
    upper = jnp.where(iota((block, block), 0) <= iota((block, block), 1), 1.0, 0.0).astype(BF16)
    carry = jnp.zeros((devices, 1), F32)
    ranks = []
    for start in range(0, columns, block):
        part = hot_b[:, start : start + block]
        inside = jnp.dot(part, upper, preferred_element_type=F32)
        here = inside + carry
        ranks.append(jnp.sum(here * hot_f[:, start : start + block], axis=0, keepdims=True))
        carry = carry + inside[:, block - 1 : block]
    rank = jnp.concatenate(ranks, axis=1).astype(jnp.int32) - 1
    place_hot = jnp.where(iota((places, columns), 0) == rank, 1.0, 0.0).astype(BF16)
    zero = jnp.zeros((1, columns), F32)
    fields = jnp.concatenate(
        [
            high.astype(F32) + 1.0,
            low.astype(F32),
            tile.astype(F32),
            gap1,
            gap2,
            gap3,
            zero,
            zero,
        ],
        axis=0,
    )
    spread = jnp.concatenate(
        [jnp.where(peer == device, fields, 0.0) for device in range(devices)], axis=0
    ).astype(BF16)
    out_ref[...] = dot_nt(spread, place_hot).astype(BF16)
    tile_hot = jnp.where(iota((tiles, columns), 0) == tile, 1.0, 0.0).astype(BF16)
    count_ref[...] = jnp.dot(
        tile_hot, jnp.ones((columns, count_ref.shape[1]), BF16), preferred_element_type=F32
    )


def arrange_kernel(devices, got_ref, meta_ref):
    places = got_ref.shape[1]
    rows = meta_ref.shape[1]
    total = jnp.zeros((5 * rows, ROWS), F32)
    row_id = iota((rows, places), 0).astype(F32) + 1.0
    low_id = iota((ROWS, places), 0).astype(F32)
    for device in range(devices):
        got = got_ref[device * FIELDS : (device + 1) * FIELDS, :].astype(F32)
        hot = got[0:1] == row_id
        zero = jnp.zeros((rows, places), F32)
        parts = [jnp.where(hot, float(device + 1), zero)]
        parts += [jnp.where(hot, got[field : field + 1], zero) for field in (2, 3, 4, 5)]
        left = jnp.concatenate(parts, axis=0).astype(BF16)
        right = jnp.where(low_id == got[1:2], 1.0, 0.0).astype(BF16)
        total = total + dot_nt(left, right)
    meta_ref[0] = total[0:rows]
    meta_ref[1] = total[rows : 2 * rows]
    meta_ref[2] = total[2 * rows : 3 * rows] + total[3 * rows : 4 * rows] + total[4 * rows :]


def tile_ranges(own, other):
    have = (own + (ROWS - 1)) // ROWS
    return jnp.maximum(own - other, 0) // (2 * ROWS), have


def network_kernel(
    devices,
    info_ref,
    state_ref,
    guest_ref,
    meta_ref,
    guest_meta_ref,
    table_ref,
    lapse_ref,
    w_in_ref,
    gains_ref,
    w_up_ref,
    w_down_ref,
    w_out_ref,
    tend_ref,
    guest_tend_ref,
    keep_ref,
    send_ref,
    wide_ref,
    hot_ref,
    total_ref,
    x_ref,
    m_ref,
):
    tiles = table_ref.shape[2]
    width = state_ref.shape[1]
    groups = devices // 2
    hidden = w_in_ref.shape[1]
    me = info_ref[2]
    given, have = tile_ranges(info_ref[0], info_ref[1])
    taken, _ = tile_ranges(info_ref[1], info_ref[0])
    own_tiles = have - given

    for group in range(groups):
        wide_ref[0:width, group * tiles : (group + 1) * tiles] = table_ref[2 * group]
        wide_ref[width : 2 * width, group * tiles : (group + 1) * tiles] = table_ref[2 * group + 1]
    total_ref[...] = jnp.zeros_like(total_ref)
    tend_ref[...] = jnp.zeros_like(tend_ref)

    def norm(values, gain):
        scale = lax.rsqrt(jnp.mean(values * values, axis=-1, keepdims=True) + 1e-06)
        return (values * scale * gain).astype(BF16)

    def one_tile(step, _):
        is_own = step < own_tiles
        index = jnp.where(is_own, step + given, step - own_tiles)
        start = pl.multiple_of(index * ROWS, ROWS)

        @pl.when(is_own)
        def _():
            x_ref[...] = state_ref[pl.ds(start, ROWS), :].astype(BF16)
            for plane in range(3):
                m_ref[plane : plane + 1, :] = meta_ref[plane, pl.ds(index, 1), :]

        @pl.when(jnp.logical_not(is_own))
        def _():
            x_ref[...] = guest_ref[pl.ds(start, ROWS), :]
            for plane in range(3):
                m_ref[plane : plane + 1, :] = guest_meta_ref[plane, pl.ds(index, 1), :]

        source = m_ref[0:1, :].astype(jnp.int32) - 1
        tile = m_ref[1:2, :]
        gap = m_ref[2:3, :]
        relative = jnp.where(source >= 0, source ^ me, -1)
        odd = (relative & 1).astype(F32)
        group_of = lax.shift_right_arithmetic(relative, 1)
        tile_id = iota((tiles, ROWS), 0).astype(F32)
        for group in range(groups):
            key = jnp.where(group_of == group, tile, -1.0)
            hot_ref[group * tiles : (group + 1) * tiles, :] = jnp.where(
                tile_id == key, 1.0, 0.0
            ).astype(BF16)
        looked = jnp.dot(wide_ref[...], hot_ref[...], preferred_element_type=F32)
        forcing = jnp.where(odd > 0.5, looked[width:, :], looked[:width, :])
        forcing = forcing + lapse_ref[...] * gap
        forcing = jnp.transpose(forcing).astype(BF16)
        inputs = jnp.concatenate([forcing, x_ref[...]], axis=1)
        h = jnp.dot(inputs, w_in_ref[...], preferred_element_type=F32)
        low = norm(h, gains_ref[0:1, :])
        up = jnp.dot(low, w_up_ref[...], preferred_element_type=F32)
        active = (up * (0.5 + 0.5 * jnp.tanh(0.5 * up))).astype(BF16)
        h = h + jnp.dot(active, w_down_ref[...], preferred_element_type=F32)
        low = norm(h, gains_ref[1:2, :])
        result = jnp.dot(low, w_out_ref[...], preferred_element_type=F32)
        tend = result[:, :width].astype(BF16)
        flux = result[:, width:].astype(BF16).astype(F32)
        odd_column = jnp.transpose(jnp.broadcast_to(odd, (8, ROWS)))[:, 0:1]
        pair = jnp.concatenate([flux * (1.0 - odd_column), flux * odd_column], axis=1)
        total_ref[...] += jnp.dot(hot_ref[...], pair.astype(BF16), preferred_element_type=F32)

        @pl.when(is_own)
        def _():
            tend_ref[pl.ds(start, ROWS), :] = tend

        @pl.when(jnp.logical_not(is_own))
        def _():
            guest_tend_ref[pl.ds(start, ROWS), :] = tend

        return 0

    lax.fori_loop(0, own_tiles + taken, one_tile, 0)
    keep_ref[...] = total_ref[:, :width]
    send_ref[...] = total_ref[:, width:].astype(BF16)


def local(
    devices,
    tile_forcing,
    elevation_gap,
    lapse_rate,
    column_tile,
    column_target,
    owner_counts,
    land_state,
    w_in,
    norm_gains,
    w_up,
    w_down,
    w_out,
):
    capacity, width = land_state.shape
    per_peer = capacity // devices + 1
    places = -(-per_peer // 128) * 128
    columns = elevation_gap.shape[0]
    tiles = tile_forcing.shape[0]
    guest_rows = -(-capacity // (2 * ROWS)) * ROWS
    meta_rows = -(-capacity // (8 * ROWS)) * 8
    bits = devices.bit_length() - 1
    me = lax.axis_index(AXES)

    def swap(values, bit):
        return lax.ppermute(values, AXES, [(i, i ^ bit) for i in range(devices)])

    other_count = swap(owner_counts, 1)
    guest_state = swap(land_state[:guest_rows].astype(BF16), 1)

    block = tile_forcing.T
    far = 1 << (bits - 3)
    gathered = jnp.stack([block] + [swap(block, s << 3) for s in range(1, far)])
    half = gathered.shape[1] // 2
    first, second = gathered[:, :half], gathered[:, half:]
    first = jnp.stack([first, swap(first, 2)], axis=1)
    second = jnp.stack([second, swap(second, 4)], axis=1)
    first = jnp.stack([first, swap(first, 4)], axis=1)
    second = jnp.stack([second, swap(second, 2)], axis=2)
    gathered = jnp.concatenate([first, second], axis=3)
    gathered = jnp.stack([gathered, swap(gathered, 1)], axis=3)
    table = gathered.reshape(devices, width, tiles)

    buckets, counts = pl.pallas_call(
        functools.partial(bucket_kernel, devices, capacity),
        out_shape=(
            jax.ShapeDtypeStruct((devices * FIELDS, places), BF16),
            jax.ShapeDtypeStruct((tiles, width), F32),
        ),
        in_specs=[VMEM] * 3,
        out_specs=(VMEM, VMEM),
        name="bucket",
    )(
        column_target.reshape(1, columns),
        column_tile.reshape(1, columns),
        elevation_gap.reshape(1, columns),
    )
    got = lax.all_to_all(
        buckets.reshape(devices, FIELDS, places), AXES, split_axis=0, concat_axis=0, tiled=True
    )
    meta = pl.pallas_call(
        functools.partial(arrange_kernel, devices),
        out_shape=jax.ShapeDtypeStruct((3, meta_rows, ROWS), F32),
        in_specs=[VMEM],
        out_specs=VMEM,
        name="arrange",
    )(got.reshape(devices * FIELDS, places))
    guest_meta = swap(meta[:, : -(-guest_rows // (8 * ROWS)) * 8], 1)
    info = jnp.concatenate([owner_counts, other_count, me.astype(jnp.int32)[None]])
    groups = devices // 2
    tend, guest_tend, keep, send = pl.pallas_call(
        functools.partial(network_kernel, devices),
        out_shape=(
            jax.ShapeDtypeStruct((capacity, width), BF16),
            jax.ShapeDtypeStruct((guest_rows, width), BF16),
            jax.ShapeDtypeStruct((groups * tiles, width), F32),
            jax.ShapeDtypeStruct((groups * tiles, width), BF16),
        ),
        in_specs=[SMEM] + [VMEM] * 11,
        out_specs=(VMEM,) * 4,
        scratch_shapes=[
            pltpu.VMEM((2 * width, groups * tiles), BF16),
            pltpu.VMEM((groups * tiles, ROWS), BF16),
            pltpu.VMEM((groups * tiles, 2 * width), F32),
            pltpu.VMEM((ROWS, width), BF16),
            pltpu.VMEM((8, ROWS), F32),
        ],
        name="network",
    )(
        info,
        land_state,
        guest_state,
        meta,
        guest_meta,
        table,
        lapse_rate.reshape(width, 1),
        w_in,
        norm_gains,
        w_up[0],
        w_down[0],
        w_out,
    )

    keep = keep.reshape(far, 2, 2, tiles, width)
    send = send.reshape(far, 2, 2, tiles, width)
    back = swap(guest_tend, 1)
    total = keep + swap(send, 1).astype(F32)
    half = tiles // 2
    first, second = total[..., :half, :], total[..., half:, :]
    first_in = swap(first[:, :, 1].astype(BF16), 2)
    second_in = swap(second[:, 1].astype(BF16), 4)
    first = first[:, :, 0] + first_in.astype(F32)
    second = second[:, 0] + second_in.astype(F32)
    first_in = swap(first[:, 1].astype(BF16), 4)
    second_in = swap(second[:, 1].astype(BF16), 2)
    first = first[:, 0] + first_in.astype(F32)
    second = second[:, 0] + second_in.astype(F32)
    total = jnp.concatenate([first, second], axis=1)
    parts = [swap(total[s].astype(BF16), s << 3) for s in range(1, far)]
    sums = total[0]
    for part in parts:
        sums = sums + part.astype(F32)
    tile_flux = sums / jnp.maximum(counts, 1.0)

    slot = jnp.arange(capacity, dtype=jnp.int32)[:, None]
    given, _ = tile_ranges(owner_counts[0], other_count[0])
    padded = jnp.pad(back, ((0, capacity - guest_rows), (0, 0)))
    change = jnp.where(slot < given * ROWS, padded, tend).astype(F32)
    new_state = jnp.where(slot < owner_counts[0], land_state + change, jnp.float32(0.0))
    return (new_state, tile_flux)


def solution(mesh):
    devices = mesh.shape["atm"] * mesh.shape["land"]
    rows, whole = P(AXES, None), P()
    return jax.shard_map(
        functools.partial(local, devices),
        mesh=mesh,
        in_specs=(rows, P(AXES), whole, P(AXES), P(AXES), P(AXES), rows) + (whole,) * 5,
        out_specs=(rows, rows),
        check_vma=False,
    )
```

```python
import functools

import jax
import jax.numpy as jnp
from jax import lax
from jax.experimental import pallas as pl
from jax.experimental.pallas import tpu as pltpu
from jax.sharding import PartitionSpec as P


AXES = ("atm", "land")
ROWS = 256
FIELDS = 8
VMEM = pl.BlockSpec(memory_space=pltpu.VMEM)
SMEM = pl.BlockSpec(memory_space=pltpu.SMEM)
BF16 = jnp.bfloat16
F32 = jnp.float32


def iota(shape, dim):
    return lax.broadcasted_iota(jnp.int32, shape, dim)


def dot_nt(a, b):
    return lax.dot_general(a, b, (((1,), (1,)), ((), ())), preferred_element_type=F32)


def cost(microseconds):
    return pl.CostEstimate(
        flops=int(microseconds * 8e6), bytes_accessed=int(microseconds * 2e6), transcendentals=0
    )


def bucket_kernel(devices, capacity, tgt_ref, tile_ref, gap_ref, out_ref, count_ref):
    columns = tgt_ref.shape[1]
    places = out_ref.shape[1]
    tiles = count_ref.shape[0]
    target = tgt_ref[...]
    peer = jnp.floor((target.astype(F32) + 0.5) * (1.0 / capacity)).astype(jnp.int32)
    slot = target - peer * capacity
    high, low = lax.shift_right_logical(slot, 8), slot & (ROWS - 1)
    tile = tile_ref[...]
    gap = gap_ref[...]
    gap1 = gap.astype(BF16).astype(F32)
    gap2 = (gap - gap1).astype(BF16).astype(F32)
    gap3 = gap - gap1 - gap2
    hot = iota((devices, columns), 0) == peer
    hot_f = jnp.where(hot, 1.0, 0.0)
    hot_b = hot_f.astype(BF16)
    block = min(256, columns)
    upper = jnp.where(iota((block, block), 0) <= iota((block, block), 1), 1.0, 0.0).astype(BF16)
    carry = jnp.zeros((devices, 1), F32)
    ranks = []
    for start in range(0, columns, block):
        part = hot_b[:, start : start + block]
        inside = jnp.dot(part, upper, preferred_element_type=F32)
        here = inside + carry
        ranks.append(jnp.sum(here * hot_f[:, start : start + block], axis=0, keepdims=True))
        carry = carry + inside[:, block - 1 : block]
    rank = jnp.concatenate(ranks, axis=1).astype(jnp.int32) - 1
    place_hot = jnp.where(iota((places, columns), 0) == rank, 1.0, 0.0).astype(BF16)
    zero = jnp.zeros((1, columns), F32)
    fields = jnp.concatenate(
        [
            high.astype(F32) + 1.0,
            low.astype(F32),
            tile.astype(F32),
            gap1,
            gap2,
            gap3,
            zero,
            zero,
        ],
        axis=0,
    )
    spread = jnp.concatenate(
        [jnp.where(peer == device, fields, 0.0) for device in range(devices)], axis=0
    ).astype(BF16)
    out_ref[...] = dot_nt(spread, place_hot).astype(BF16)
    tile_hot = jnp.where(iota((tiles, columns), 0) == tile, 1.0, 0.0).astype(BF16)
    count_ref[...] = jnp.dot(
        tile_hot, jnp.ones((columns, count_ref.shape[1]), BF16), preferred_element_type=F32
    )


def arrange_kernel(devices, tiles, me_ref, got_ref, mine_ref, guest_ref):
    places = got_ref.shape[1]
    rows = mine_ref.shape[1]
    total = jnp.zeros((5 * rows, ROWS), F32)
    row_id = iota((rows, places), 0).astype(F32) + 1.0
    low_id = iota((ROWS, places), 0).astype(F32)
    for device in range(devices):
        got = got_ref[device * FIELDS : (device + 1) * FIELDS, :].astype(F32)
        hot = got[0:1] == row_id
        zero = jnp.zeros((rows, places), F32)
        parts = [jnp.where(hot, float(device + 1), zero)]
        parts += [jnp.where(hot, got[field : field + 1], zero) for field in (2, 3, 4, 5)]
        left = jnp.concatenate(parts, axis=0).astype(BF16)
        right = jnp.where(low_id == got[1:2], 1.0, 0.0).astype(BF16)
        total = total + dot_nt(left, right)
    source = total[0:rows].astype(jnp.int32) - 1
    tile = total[rows : 2 * rows].astype(jnp.int32)
    gap = total[2 * rows : 3 * rows] + total[3 * rows : 4 * rows] + total[4 * rows :]
    for out_ref, me in ((mine_ref, me_ref[0]), (guest_ref, me_ref[0] ^ 1)):
        row = table_row(devices, tiles, source ^ me, tile)
        out_ref[0] = jnp.where(source >= 0, row, devices * tiles).astype(F32)
        out_ref[1] = gap


def table_row(devices, tiles, relative, tile):
    groups, half = devices // 2, tiles // 2
    far = groups // 4
    group = (lax.shift_right_logical(relative, 1) & 3) * far + lax.shift_right_logical(relative, 3)
    part = jnp.where(tile >= half, 1, 0)
    return (relative & 1) * (groups * tiles) + part * (groups * half) + group * half + (tile - part * half)


def tile_ranges(own, other):
    have = (own + (ROWS - 1)) // ROWS
    return jnp.maximum(own - other, 0) // (2 * ROWS), have


def network_kernel(
    own_ref,
    other_ref,
    state_ref,
    guest_ref,
    mine_ref,
    guest_mine_ref,
    even_ref,
    odd_ref,
    lapse_ref,
    w_in_ref,
    gains_ref,
    w_up_ref,
    w_down_ref,
    w_out_ref,
    tend_ref,
    guest_tend_ref,
    keep_ref,
    send_ref,
    table_ref,
    first_ref,
    second_ref,
    rows_ref,
    flux_ref,
    x_ref,
    gap_ref,
    index_ref,
    scalar_ref,
    sem,
):
    half = even_ref.shape[0]
    width = even_ref.shape[1]
    spare = 2 * half
    given, have = tile_ranges(own_ref[0], other_ref[0])
    taken, _ = tile_ranges(other_ref[0], own_ref[0])
    own_tiles = have - given
    all_tiles = own_tiles + taken
    lines = mine_ref.shape[1]
    last_line = 2 * lines

    index_ref[0:lines, :] = mine_ref[0].astype(jnp.int32)
    index_ref[lines:last_line, :] = guest_mine_ref[0].astype(jnp.int32)
    index_ref[last_line:, :] = jnp.full_like(index_ref[last_line:, :], spare)
    copy = pltpu.make_async_copy(index_ref, scalar_ref, sem)
    copy.start()
    table_ref[0:half, :] = even_ref[...].astype(F32)
    table_ref[half:spare, :] = odd_ref[...].astype(F32)
    table_ref[spare:, :] = jnp.zeros_like(table_ref[spare:, :])
    first_ref[...] = jnp.zeros_like(first_ref)
    second_ref[...] = jnp.zeros_like(second_ref)
    copy.wait()

    def norm(values, gain):
        scale = lax.rsqrt(jnp.mean(values * values, axis=-1, keepdims=True) + 1e-06)
        return (values * scale * gain).astype(BF16)

    def place_of(step):
        is_own = step < own_tiles
        index = jnp.where(is_own, step + given, step - own_tiles)
        index = jnp.where(step < all_tiles, index, 0)
        return is_own, index, pl.multiple_of(index * ROWS, ROWS)

    def line_of(step):
        is_own, index, _ = place_of(step)
        line = jnp.where(is_own, index, index + lines)
        return jnp.where((step >= 0) & (step < all_tiles), line, last_line)

    def fetch(step):
        for chain in range(2):
            line = line_of(2 * step + chain)
            for row in range(ROWS):
                at = chain * ROWS + row
                rows_ref[at : at + 1, :] = table_ref[pl.ds(scalar_ref[line, row], 1), :]

    def spread(step):
        for chain in range(2):
            line = line_of(2 * step + chain)
            for row in range(ROWS):
                at = chain * ROWS + row
                bank = second_ref if row % 2 else first_ref
                where = pl.ds(scalar_ref[line, row], 1)
                bank[where, :] = bank[where, :] + flux_ref[at : at + 1, :]

    def load(chain, step):
        is_own, index, start = place_of(step)

        @pl.when(is_own)
        def _():
            x_ref[chain] = state_ref[pl.ds(start, ROWS), :].astype(BF16)
            gap_ref[chain] = jnp.broadcast_to(mine_ref[1, pl.ds(index, 1), :], (8, ROWS))

        @pl.when(jnp.logical_not(is_own))
        def _():
            x_ref[chain] = guest_ref[pl.ds(start, ROWS), :]
            gap_ref[chain] = jnp.broadcast_to(guest_mine_ref[1, pl.ds(index, 1), :], (8, ROWS))

    def store(step, tend):
        is_own, _, start = place_of(step)

        @pl.when(is_own)
        def _():
            tend_ref[pl.ds(start, ROWS), :] = tend

        @pl.when(jnp.logical_not(is_own) & (step < all_tiles))
        def _():
            guest_tend_ref[pl.ds(start, ROWS), :] = tend

    def two_tiles(step, _):
        chains = range(2)
        for chain in chains:
            load(chain, 2 * step + chain)
        inputs = []
        for chain in chains:
            gap = jnp.transpose(gap_ref[chain])[:, 0:1]
            forcing = rows_ref[chain * ROWS : (chain + 1) * ROWS, :] + gap * lapse_ref[...]
            inputs.append(jnp.concatenate([forcing.astype(BF16), x_ref[chain]], axis=1))
        fetch(step + 1)
        spread(step - 1)
        h = [jnp.dot(v, w_in_ref[...], preferred_element_type=F32) for v in inputs]
        low = [norm(v, gains_ref[0:1, :]) for v in h]
        up = [jnp.dot(v, w_up_ref[...], preferred_element_type=F32) for v in low]
        active = [(v * (0.5 + 0.5 * jnp.tanh(0.5 * v))).astype(BF16) for v in up]
        h = [
            v + jnp.dot(a, w_down_ref[...], preferred_element_type=F32) for v, a in zip(h, active)
        ]
        low = [norm(v, gains_ref[1:2, :]) for v in h]
        result = [jnp.dot(v, w_out_ref[...], preferred_element_type=F32) for v in low]
        for chain in chains:
            flux_ref[chain * ROWS : (chain + 1) * ROWS, :] = (
                result[chain][:, width:].astype(BF16).astype(F32)
            )
        for chain in chains:
            store(2 * step + chain, result[chain][:, :width].astype(BF16))
        return 0

    steps = (all_tiles + 1) // 2
    fetch(0)
    lax.fori_loop(0, steps, two_tiles, 0)
    spread(steps - 1)
    keep_ref[...] = first_ref[0:half, :] + second_ref[0:half, :]
    send_ref[...] = (first_ref[half:spare, :] + second_ref[half:spare, :]).astype(BF16)


def add_near(keep_ref, in_ref, first_ref, first_out_ref, second_ref, second_out_ref):
    for other in range(2):
        first_ref[other] = keep_ref[0, other, 0] + in_ref[0, other, 0].astype(F32)
        second_ref[other] = keep_ref[1, 0, other] + in_ref[1, 0, other].astype(F32)
        first_out_ref[other] = (keep_ref[0, other, 1] + in_ref[0, other, 1].astype(F32)).astype(BF16)
        second_out_ref[other] = (keep_ref[1, 1, other] + in_ref[1, 1, other].astype(F32)).astype(BF16)


def add_next(a_ref, a_in_ref, b_ref, b_in_ref, first_ref, first_out_ref, second_ref, second_out_ref):
    first_ref[...] = a_ref[0] + a_in_ref[0].astype(F32)
    second_ref[...] = b_ref[0] + b_in_ref[0].astype(F32)
    first_out_ref[...] = (a_ref[1] + a_in_ref[1].astype(F32)).astype(BF16)
    second_out_ref[...] = (b_ref[1] + b_in_ref[1].astype(F32)).astype(BF16)


def add_far(a_ref, a_in_ref, b_ref, b_in_ref, sum_ref, *out_refs):
    half = a_ref.shape[1]
    for far, out_ref in enumerate((sum_ref,) + out_refs):
        out_ref[0:half, :] = (a_ref[far] + a_in_ref[far].astype(F32)).astype(out_ref.dtype)
        out_ref[half:, :] = (b_ref[far] + b_in_ref[far].astype(F32)).astype(out_ref.dtype)


def local(
    devices,
    tile_forcing,
    elevation_gap,
    lapse_rate,
    column_tile,
    column_target,
    owner_counts,
    land_state,
    w_in,
    norm_gains,
    w_up,
    w_down,
    w_out,
):
    capacity, width = land_state.shape
    per_peer = capacity // devices + 1
    places = -(-per_peer // 128) * 128
    columns = elevation_gap.shape[0]
    tiles = tile_forcing.shape[0]
    guest_rows = -(-capacity // (2 * ROWS)) * ROWS
    meta_rows = -(-capacity // (8 * ROWS)) * 8
    bits = devices.bit_length() - 1
    me = lax.axis_index(AXES)

    def swap(values, bit):
        return lax.ppermute(values, AXES, [(i, i ^ bit) for i in range(devices)])

    small = pltpu.CompilerParams(vmem_limit_bytes=24 << 20)
    buckets, counts = pl.pallas_call(
        functools.partial(bucket_kernel, devices, capacity),
        out_shape=(
            jax.ShapeDtypeStruct((devices * FIELDS, places), BF16),
            jax.ShapeDtypeStruct((tiles, width), F32),
        ),
        in_specs=[VMEM] * 3,
        out_specs=(VMEM, VMEM),
        cost_estimate=cost(4.0),
        compiler_params=small,
        name="bucket",
    )(
        column_target.reshape(1, columns),
        column_tile.reshape(1, columns),
        elevation_gap.reshape(1, columns),
    )
    got = lax.all_to_all(
        buckets.reshape(devices, FIELDS, places), AXES, split_axis=0, concat_axis=0, tiled=True
    )
    tile_forcing, counts, mine = lax.optimization_barrier((tile_forcing, counts, owner_counts))

    far = 1 << (bits - 3)
    half = tiles // 2
    gathered = [tile_forcing] + [swap(tile_forcing, s << 3) for s in range(1, far)]
    first = jnp.stack([piece[:half] for piece in gathered])
    second = jnp.stack([piece[half:] for piece in gathered])
    first = jnp.stack([first, swap(first, 2)])
    second = jnp.stack([second, swap(second, 4)])
    first = jnp.stack([first, swap(first, 4)])
    second = jnp.stack([second, swap(second, 2)], axis=1)
    groups = devices // 2
    even = jnp.stack([first, second]).reshape(groups * tiles, width)
    odd = swap(even, 1)

    other_count = swap(mine, 1)
    guest_state = swap(land_state[:guest_rows].astype(BF16), 1)

    mine, theirs = pl.pallas_call(
        functools.partial(arrange_kernel, devices, tiles),
        out_shape=(jax.ShapeDtypeStruct((2, meta_rows, ROWS), F32),) * 2,
        in_specs=[SMEM, VMEM],
        out_specs=(VMEM,) * 2,
        cost_estimate=cost(4.0),
        compiler_params=small,
        name="arrange",
    )(me.astype(jnp.int32)[None], got.reshape(devices * FIELDS, places))
    guest_mine = swap(theirs, 1)
    table_rows = devices * tiles
    network_bytes = (
        (12 << 20)
        + (capacity + guest_rows) * width * 8
        + (w_in.size + w_up.size + w_down.size + w_out.size) * 2
        + table_rows * width * 18
    )
    network_bytes = min(network_bytes, 60 * 1024 * 1024)
    tend, guest_tend, keep, send = pl.pallas_call(
        network_kernel,
        out_shape=(
            jax.ShapeDtypeStruct((capacity, width), BF16),
            jax.ShapeDtypeStruct((guest_rows, width), BF16),
            jax.ShapeDtypeStruct((groups * tiles, width), F32),
            jax.ShapeDtypeStruct((groups * tiles, width), BF16),
        ),
        in_specs=[SMEM] * 2 + [VMEM] * 12,
        out_specs=(VMEM,) * 4,
        scratch_shapes=[
            pltpu.VMEM((table_rows + 8, width), F32),
            pltpu.VMEM((table_rows + 8, width), F32),
            pltpu.VMEM((table_rows + 8, width), F32),
            pltpu.VMEM((2 * ROWS, width), F32),
            pltpu.VMEM((2 * ROWS, width), F32),
            pltpu.VMEM((2, ROWS, width), BF16),
            pltpu.VMEM((2, 8, ROWS), F32),
            pltpu.VMEM((2 * meta_rows + 8, ROWS), jnp.int32),
            pltpu.SMEM((2 * meta_rows + 8, ROWS), jnp.int32),
            pltpu.SemaphoreType.DMA,
        ],
        cost_estimate=cost(50.0),
        compiler_params=pltpu.CompilerParams(vmem_limit_bytes=network_bytes),
        name="network",
    )(
        owner_counts,
        other_count,
        land_state,
        guest_state,
        mine,
        guest_mine,
        even,
        odd,
        lapse_rate.reshape(1, width),
        w_in,
        norm_gains,
        w_up[0],
        w_down[0],
        w_out,
    )
    back = swap(guest_tend, 1)

    def add(kernel, shapes, *arrays):
        return pl.pallas_call(
            kernel,
            out_shape=tuple(jax.ShapeDtypeStruct(shape, dtype) for shape, dtype in shapes),
            in_specs=[VMEM] * len(arrays),
            out_specs=(VMEM,) * len(shapes),
            cost_estimate=cost(0.5),
            compiler_params=small,
            name="add",
        )(*arrays)

    shape = (2, 2, 2, far, half, width)
    block = (2, far, half, width)
    first, first_out, second, second_out = add(
        add_near, [(block, F32), (block, BF16)] * 2, keep.reshape(shape), swap(send.reshape(shape), 1)
    )
    block = (far, half, width)
    first, first_out, second, second_out = add(
        add_next,
        [(block, F32), (block, BF16)] * 2,
        first,
        swap(first_out, 2),
        second,
        swap(second_out, 4),
    )
    block = (tiles, width)
    sums, *parts = add(
        add_far,
        [(block, F32)] + [(block, BF16)] * (far - 1),
        first,
        swap(first_out, 4),
        second,
        swap(second_out, 2),
    )
    parts = [swap(part, s << 3) for s, part in zip(range(1, far), parts)]
    for part in parts:
        sums = sums + part.astype(F32)
    tile_flux = sums / jnp.maximum(counts, 1.0)

    slot = jnp.arange(capacity, dtype=jnp.int32)[:, None]
    given, _ = tile_ranges(owner_counts[0], other_count[0])
    padded = jnp.pad(back, ((0, capacity - guest_rows), (0, 0)))
    change = jnp.where(slot < given * ROWS, padded, tend).astype(F32)
    new_state = jnp.where(slot < owner_counts[0], land_state + change, jnp.float32(0.0))
    return (new_state, tile_flux)


def solution(mesh):
    devices = mesh.shape["atm"] * mesh.shape["land"]
    rows, whole = P(AXES, None), P()

    def body(*arrays):
        return local(devices, *arrays)

    return jax.shard_map(
        body,
        mesh=mesh,
        in_specs=(rows, P(AXES), whole, P(AXES), P(AXES), P(AXES), rows) + (whole,) * 5,
        out_specs=(rows, rows),
        check_vma=False,
    )
```

```python
import functools

import jax
import jax.numpy as jnp
from jax import lax
from jax.experimental import pallas as pl
from jax.experimental.pallas import tpu as pltpu
from jax.sharding import PartitionSpec as P


AXES = ("atm", "land")
ROWS = 256
FIELDS = 8
VMEM = pl.BlockSpec(memory_space=pltpu.VMEM)
SMEM = pl.BlockSpec(memory_space=pltpu.SMEM)
HBM = pl.BlockSpec(memory_space=pltpu.HBM)
BF16 = jnp.bfloat16
F32 = jnp.float32


def iota(shape, dim):
    return lax.broadcasted_iota(jnp.int32, shape, dim)


def dot_nt(a, b):
    return lax.dot_general(a, b, (((1,), (1,)), ((), ())), preferred_element_type=F32)


def hbm(array):
    return pltpu.with_memory_space_constraint(array, pltpu.HBM)


def vmem(array):
    return pltpu.with_memory_space_constraint(array, pltpu.VMEM)


def cost(microseconds):
    return pl.CostEstimate(
        flops=int(microseconds * 8e6), bytes_accessed=int(microseconds * 2e6), transcendentals=0
    )


def bucket_kernel(
    devices,
    capacity,
    tgt_hbm,
    tile_hbm,
    gap_hbm,
    out_ref,
    count_ref,
    tgt_ref,
    tile_ref,
    gap_ref,
    sems,
):
    pairs = ((tgt_hbm, tgt_ref), (tile_hbm, tile_ref), (gap_hbm, gap_ref))
    copies = [pltpu.make_async_copy(*pair, sems.at[place]) for place, pair in enumerate(pairs)]
    for copy in copies:
        copy.start()
    for copy in copies:
        copy.wait()
    columns = tgt_ref.shape[1]
    places = out_ref.shape[1]
    tiles = count_ref.shape[0]
    target = tgt_ref[...]
    peer = jnp.floor((target.astype(F32) + 0.5) * (1.0 / capacity)).astype(jnp.int32)
    slot = target - peer * capacity
    high, low = lax.shift_right_logical(slot, 8), slot & (ROWS - 1)
    tile = tile_ref[...]
    gap = gap_ref[...]
    gap1 = gap.astype(BF16).astype(F32)
    gap2 = (gap - gap1).astype(BF16).astype(F32)
    gap3 = gap - gap1 - gap2
    hot = iota((devices, columns), 0) == peer
    hot_f = jnp.where(hot, 1.0, 0.0)
    hot_b = hot_f.astype(BF16)
    block = min(256, columns)
    upper = jnp.where(iota((block, block), 0) <= iota((block, block), 1), 1.0, 0.0).astype(BF16)
    carry = jnp.zeros((devices, 1), F32)
    ranks = []
    for start in range(0, columns, block):
        part = hot_b[:, start : start + block]
        inside = jnp.dot(part, upper, preferred_element_type=F32)
        here = inside + carry
        ranks.append(jnp.sum(here * hot_f[:, start : start + block], axis=0, keepdims=True))
        carry = carry + inside[:, block - 1 : block]
    rank = jnp.concatenate(ranks, axis=1).astype(jnp.int32) - 1
    place_hot = jnp.where(iota((places, columns), 0) == rank, 1.0, 0.0).astype(BF16)
    zero = jnp.zeros((1, columns), F32)
    fields = jnp.concatenate(
        [
            high.astype(F32) + 1.0,
            low.astype(F32),
            tile.astype(F32),
            gap1,
            gap2,
            gap3,
            zero,
            zero,
        ],
        axis=0,
    )
    spread = jnp.concatenate(
        [jnp.where(peer == device, fields, 0.0) for device in range(devices)], axis=0
    ).astype(BF16)
    out_ref[...] = dot_nt(spread, place_hot).astype(BF16)
    tile_hot = jnp.where(iota((tiles, columns), 0) == tile, 1.0, 0.0).astype(BF16)
    count_ref[...] = jnp.dot(
        tile_hot, jnp.ones((columns, count_ref.shape[1]), BF16), preferred_element_type=F32
    )


def arrange_kernel(devices, tiles, me_ref, got_ref, weight_hbms, mine_ref, guest_ref, weight_refs, sems):
    pairs = zip(weight_hbms, weight_refs)
    copies = [pltpu.make_async_copy(*pair, sems.at[place]) for place, pair in enumerate(pairs)]
    for copy in copies:
        copy.start()
    places = got_ref.shape[1]
    rows = mine_ref.shape[1]
    total = jnp.zeros((5 * rows, ROWS), F32)
    row_id = iota((rows, places), 0).astype(F32) + 1.0
    low_id = iota((ROWS, places), 0).astype(F32)
    for device in range(devices):
        got = got_ref[device * FIELDS : (device + 1) * FIELDS, :].astype(F32)
        hot = got[0:1] == row_id
        zero = jnp.zeros((rows, places), F32)
        parts = [jnp.where(hot, float(device + 1), zero)]
        parts += [jnp.where(hot, got[field : field + 1], zero) for field in (2, 3, 4, 5)]
        left = jnp.concatenate(parts, axis=0).astype(BF16)
        right = jnp.where(low_id == got[1:2], 1.0, 0.0).astype(BF16)
        total = total + dot_nt(left, right)
    source = total[0:rows].astype(jnp.int32) - 1
    tile = total[rows : 2 * rows].astype(jnp.int32)
    gap = total[2 * rows : 3 * rows] + total[3 * rows : 4 * rows] + total[4 * rows :]
    for out_ref, me in ((mine_ref, me_ref[0]), (guest_ref, me_ref[0] ^ 1)):
        row = table_row(devices, tiles, source ^ me, tile)
        out_ref[0] = jnp.where(source >= 0, row, devices * tiles).astype(F32)
        out_ref[1] = gap
    for copy in copies:
        copy.wait()


def table_row(devices, tiles, relative, tile):
    groups, half = devices // 2, tiles // 2
    far = groups // 4
    group = (lax.shift_right_logical(relative, 1) & 3) * far + lax.shift_right_logical(relative, 3)
    part = jnp.where(tile >= half, 1, 0)
    return (relative & 1) * (groups * tiles) + part * (groups * half) + group * half + (tile - part * half)


def tile_ranges(own, other):
    have = (own + (ROWS - 1)) // ROWS
    return jnp.maximum(own - other, 0) // (2 * ROWS), have


def network_kernel(
    own_ref,
    other_ref,
    state_ref,
    guest_ref,
    mine_ref,
    guest_mine_ref,
    even_refs,
    odd_refs,
    lapse_ref,
    gains_ref,
    w_in_ref,
    w_up_ref,
    w_down_ref,
    w_out_ref,
    tend_ref,
    guest_tend_ref,
    keep_ref,
    send_ref,
    table_ref,
    bank_refs,
    rows_ref,
    flux_ref,
    x_ref,
    gap_ref,
    index_ref,
    scalar_ref,
    out_ref,
    sem,
    out_sems,
):
    half, width = keep_ref.shape
    spare = 2 * half
    given, have = tile_ranges(own_ref[0], other_ref[0])
    taken, _ = tile_ranges(other_ref[0], own_ref[0])
    own_tiles = have - given
    all_tiles = own_tiles + taken
    lines = mine_ref.shape[1]
    last_line = 2 * lines
    guest_rows = guest_ref.shape[0]
    lanes = index_ref.shape[1]
    parts = ROWS // lanes
    part_lines = last_line + 8

    for part in range(parts):
        side = slice(part * lanes, (part + 1) * lanes)
        base = part * part_lines
        index_ref[base : base + lines, :] = mine_ref[0, :, side].astype(jnp.int32)
        index_ref[base + lines : base + last_line, :] = guest_mine_ref[0, :, side].astype(jnp.int32)
        index_ref[base + last_line : base + part_lines, :] = jnp.full((8, lanes), spare, jnp.int32)
    copy = pltpu.make_async_copy(index_ref, scalar_ref, sem)
    copy.start()
    for core, pieces in enumerate((even_refs, odd_refs)):
        base = core * half
        run = pieces[0].shape[1] * pieces[0].shape[2]
        for part, piece in enumerate(pieces):
            for other in range(2):
                y, x = (part % 2, other) if part < 2 else (other, part % 2)
                at = base + (part // 2) * (half // 2) + (2 * y + x) * run
                table_ref[at : at + run, :] = piece[other].astype(F32).reshape(run, width)
    table_ref[spare:, :] = jnp.zeros_like(table_ref[spare:, :])
    for bank in bank_refs:
        bank[...] = jnp.zeros_like(bank)
    copy.wait()

    def norm(values, gain):
        scale = lax.rsqrt(jnp.mean(values * values, axis=-1, keepdims=True) + 1e-06)
        return (values * scale * gain).astype(BF16)

    def place_of(step):
        is_own = step < own_tiles
        index = jnp.where(is_own, step + given, step - own_tiles)
        index = jnp.where(step < all_tiles, index, 0)
        return is_own, index, pl.multiple_of(index * ROWS, ROWS)

    def line_of(step):
        is_own, index, _ = place_of(step)
        line = jnp.where(is_own, index, index + lines)
        return jnp.where((step >= 0) & (step < all_tiles), line, last_line)

    def fetch(step):
        for chain in range(2):
            line = line_of(2 * step + chain)
            for row in range(ROWS):
                at = chain * ROWS + row
                where = scalar_ref[line + row // lanes * part_lines, row % lanes]
                rows_ref[at : at + 1, :] = table_ref[pl.ds(where, 1), :]

    def spread(step):
        for chain in range(2):
            line = line_of(2 * step + chain)
            for row in range(ROWS):
                at = chain * ROWS + row
                bank = bank_refs[row % len(bank_refs)]
                where = pl.ds(scalar_ref[line + row // lanes * part_lines, row % lanes], 1)
                bank[where, :] = bank[where, :] + flux_ref[at : at + 1, :]

    def load(chain, step):
        is_own, index, start = place_of(step)

        @pl.when(is_own)
        def _():
            x_ref[chain] = state_ref[pl.ds(start, ROWS), :].astype(BF16)
            gap_ref[chain] = jnp.broadcast_to(mine_ref[1, pl.ds(index, 1), :], (8, ROWS))

        @pl.when(jnp.logical_not(is_own))
        def _():
            x_ref[chain] = guest_ref[pl.ds(start, ROWS), :]
            gap_ref[chain] = jnp.broadcast_to(guest_mine_ref[1, pl.ds(index, 1), :], (8, ROWS))

    def store(chain, step, tend):
        is_own, _, start = place_of(step)
        start = pl.multiple_of(jnp.where(step < all_tiles, start, guest_rows), ROWS)

        @pl.when(step >= 2)
        def _():
            arrived(chain)

        out_ref[chain] = tend

        @pl.when(is_own)
        def _():
            pltpu.make_async_copy(
                out_ref.at[chain], tend_ref.at[pl.ds(start, ROWS)], out_sems.at[chain]
            ).start()

        @pl.when(jnp.logical_not(is_own))
        def _():
            pltpu.make_async_copy(
                out_ref.at[chain], guest_tend_ref.at[pl.ds(start, ROWS)], out_sems.at[chain]
            ).start()

    def arrived(chain):
        pltpu.make_async_copy(
            out_ref.at[chain], tend_ref.at[pl.ds(0, ROWS)], out_sems.at[chain]
        ).wait()

    def two_tiles(step, _):
        chains = range(2)
        for chain in chains:
            load(chain, 2 * step + chain)
        inputs = []
        for chain in chains:
            gap = jnp.transpose(gap_ref[chain])[:, 0:1]
            forcing = rows_ref[chain * ROWS : (chain + 1) * ROWS, :] + gap * lapse_ref[...]
            inputs.append(jnp.concatenate([forcing.astype(BF16), x_ref[chain]], axis=1))
        fetch(step + 1)
        spread(step - 1)
        h = [jnp.dot(v, w_in_ref[...], preferred_element_type=F32) for v in inputs]
        low = [norm(v, gains_ref[0:1, :]) for v in h]
        up = [jnp.dot(v, w_up_ref[...], preferred_element_type=F32) for v in low]
        active = [(v * (0.5 + 0.5 * jnp.tanh(0.5 * v))).astype(BF16) for v in up]
        h = [
            v + jnp.dot(a, w_down_ref[...], preferred_element_type=F32) for v, a in zip(h, active)
        ]
        low = [norm(v, gains_ref[1:2, :]) for v in h]
        result = [jnp.dot(v, w_out_ref[...], preferred_element_type=F32) for v in low]
        for chain in chains:
            flux_ref[chain * ROWS : (chain + 1) * ROWS, :] = (
                result[chain][:, width:].astype(BF16).astype(F32)
            )
        for chain in chains:
            store(chain, 2 * step + chain, result[chain][:, :width].astype(BF16))
        return 0

    steps = (all_tiles + 1) // 2
    fetch(0)
    lax.fori_loop(0, steps, two_tiles, 0)
    spread(steps - 1)
    chunk = min(half, 128)

    def gather(place, _):
        low = pl.ds(pl.multiple_of(place * chunk, chunk), chunk)
        high = pl.ds(pl.multiple_of(half + place * chunk, chunk), chunk)
        keep_ref[low, :] = functools.reduce(jnp.add, [bank[low, :] for bank in bank_refs])
        sums = functools.reduce(jnp.add, [bank[high, :] for bank in bank_refs])
        send_ref[low, :] = sums.astype(BF16)
        return 0

    lax.fori_loop(0, half // chunk, gather, 0)
    for chain in range(2):
        arrived(chain)


def finish_kernel(own_ref, other_ref, state_ref, tend_ref, back_ref, out_ref):
    own = own_ref[0]
    given, _ = tile_ranges(own, other_ref[0])
    rows = out_ref.shape[0]
    slot = iota((rows, 1), 0) + pl.program_id(0) * rows
    change = jnp.where(slot < given * ROWS, back_ref[...].astype(F32), tend_ref[...].astype(F32))
    out_ref[...] = jnp.where(slot < own, state_ref[...] + change, 0.0)


def add_near(keep_ref, in_ref, first_ref, first_out_ref, second_ref, second_out_ref):
    for other in range(2):
        first_ref[other] = keep_ref[0, other, 0] + in_ref[0, other, 0].astype(F32)
        second_ref[other] = keep_ref[1, 0, other] + in_ref[1, 0, other].astype(F32)
        first_out_ref[other] = (keep_ref[0, other, 1] + in_ref[0, other, 1].astype(F32)).astype(BF16)
        second_out_ref[other] = (keep_ref[1, 1, other] + in_ref[1, 1, other].astype(F32)).astype(BF16)


def add_next(a_ref, a_in_ref, b_ref, b_in_ref, first_ref, first_out_ref, second_ref, second_out_ref):
    first_ref[...] = a_ref[0] + a_in_ref[0].astype(F32)
    second_ref[...] = b_ref[0] + b_in_ref[0].astype(F32)
    first_out_ref[...] = (a_ref[1] + a_in_ref[1].astype(F32)).astype(BF16)
    second_out_ref[...] = (b_ref[1] + b_in_ref[1].astype(F32)).astype(BF16)


def add_far(a_ref, a_in_ref, b_ref, b_in_ref, sum_ref, *out_refs):
    half = a_ref.shape[1]
    for far, out_ref in enumerate((sum_ref,) + out_refs):
        out_ref[0:half, :] = (a_ref[far] + a_in_ref[far].astype(F32)).astype(out_ref.dtype)
        out_ref[half:, :] = (b_ref[far] + b_in_ref[far].astype(F32)).astype(out_ref.dtype)


def local(
    devices,
    tile_forcing,
    elevation_gap,
    lapse_rate,
    column_tile,
    column_target,
    owner_counts,
    land_state,
    w_in,
    norm_gains,
    w_up,
    w_down,
    w_out,
):
    capacity, width = land_state.shape
    per_peer = capacity // devices + 1
    places = -(-per_peer // 128) * 128
    columns = elevation_gap.shape[0]
    tiles = tile_forcing.shape[0]
    guest_rows = -(-capacity // (2 * ROWS)) * ROWS
    meta_rows = -(-capacity // (8 * ROWS)) * 8
    bits = devices.bit_length() - 1
    me = lax.axis_index(AXES)

    def swap(values, bit):
        return lax.ppermute(values, AXES, [(i, i ^ bit) for i in range(devices)])

    small = pltpu.CompilerParams(vmem_limit_bytes=24 << 20)
    buckets, counts = pl.pallas_call(
        functools.partial(bucket_kernel, devices, capacity),
        out_shape=(
            jax.ShapeDtypeStruct((devices * FIELDS, places), BF16),
            jax.ShapeDtypeStruct((tiles, width), F32),
        ),
        in_specs=[HBM] * 3,
        out_specs=(VMEM,) * 2,
        scratch_shapes=[
            pltpu.VMEM((1, columns), jnp.int32),
            pltpu.VMEM((1, columns), jnp.int32),
            pltpu.VMEM((1, columns), F32),
            pltpu.SemaphoreType.DMA((3,)),
        ],
        cost_estimate=cost(3.0),
        compiler_params=small,
        name="bucket",
    )(
        hbm(column_target.reshape(1, columns)),
        hbm(column_tile.reshape(1, columns)),
        hbm(elevation_gap.reshape(1, columns)),
    )
    got = lax.all_to_all(
        buckets.reshape(devices, FIELDS, places), AXES, split_axis=0, concat_axis=0, tiled=True
    )
    far = 1 << (bits - 3)
    half = tiles // 2
    gathered = [tile_forcing] + [swap(tile_forcing, s << 3) for s in range(1, far)]
    first = jnp.stack([piece[:half] for piece in gathered])
    second = jnp.stack([piece[half:] for piece in gathered])
    first = jnp.stack([first, swap(first, 2)])
    second = jnp.stack([second, swap(second, 4)])
    even = (first, swap(first, 4), second, swap(second, 2))
    groups = devices // 2
    odd = tuple(swap(piece, 1) for piece in even)

    other_count = swap(owner_counts, 1)
    guest_state = swap(land_state[:guest_rows].astype(BF16), 1)

    weights = (w_in, w_up[0], w_down[0], w_out)
    mine, theirs, weights = pl.pallas_call(
        functools.partial(arrange_kernel, devices, tiles),
        out_shape=(jax.ShapeDtypeStruct((2, meta_rows, ROWS), F32),) * 2
        + (tuple(jax.ShapeDtypeStruct(w.shape, BF16) for w in weights),),
        in_specs=[SMEM, VMEM, (HBM,) * 4],
        out_specs=(VMEM, VMEM, (VMEM,) * 4),
        scratch_shapes=[pltpu.SemaphoreType.DMA((4,))],
        cost_estimate=cost(4.0),
        compiler_params=small,
        name="arrange",
    )(
        me.astype(jnp.int32)[None],
        got.reshape(devices * FIELDS, places),
        tuple(hbm(w) for w in weights),
    )
    guest_mine = swap(theirs, 1)
    table_rows = devices * tiles
    held = vmem if table_rows <= 8192 else hbm
    network_bytes = (
        (12 << 20)
        + (capacity + guest_rows) * width * 8
        + table_rows * width * (4 * (5 if table_rows <= 8192 else 2) + 10)
    )
    if table_rows > 8192:
        network_bytes = 60 * 1024 * 1024
    tend, guest_tend, keep, send = pl.pallas_call(
        network_kernel,
        out_shape=(
            jax.ShapeDtypeStruct((capacity, width), BF16),
            jax.ShapeDtypeStruct((guest_rows + ROWS, width), BF16),
            jax.ShapeDtypeStruct((groups * tiles, width), F32),
            jax.ShapeDtypeStruct((groups * tiles, width), BF16),
        ),
        in_specs=[SMEM] * 2 + [VMEM] * 4 + [(VMEM,) * 4] * 2 + [VMEM] * 6,
        out_specs=(HBM, HBM, VMEM, VMEM),
        scratch_shapes=[
            pltpu.VMEM((table_rows + 8, width), F32),
            [pltpu.VMEM((table_rows + 8, width), F32)] * (4 if table_rows <= 8192 else 1),
            pltpu.VMEM((2 * ROWS, width), F32),
            pltpu.VMEM((2 * ROWS, width), F32),
            pltpu.VMEM((2, ROWS, width), BF16),
            pltpu.VMEM((2, 8, ROWS), F32),
            pltpu.VMEM((ROWS // width * (2 * meta_rows + 8), width), jnp.int32),
            pltpu.SMEM((ROWS // width * (2 * meta_rows + 8), width), jnp.int32),
            pltpu.VMEM((2, ROWS, width), BF16),
            pltpu.SemaphoreType.DMA,
            pltpu.SemaphoreType.DMA((2,)),
        ],
        cost_estimate=cost(50.0),
        compiler_params=pltpu.CompilerParams(vmem_limit_bytes=network_bytes),
        name="network",
    )(
        owner_counts,
        other_count,
        land_state,
        guest_state,
        mine,
        guest_mine,
        tuple(held(piece) for piece in even),
        tuple(held(piece) for piece in odd),
        lapse_rate.reshape(1, width),
        norm_gains,
        *(held(w) for w in weights),
    )
    back = swap(guest_tend, 1)

    def add(kernel, shapes, *arrays):
        return pl.pallas_call(
            kernel,
            out_shape=tuple(jax.ShapeDtypeStruct(shape, dtype) for shape, dtype in shapes),
            in_specs=[VMEM] * len(arrays),
            out_specs=(VMEM,) * len(shapes),
            cost_estimate=cost(0.5),
            compiler_params=small,
            name="add",
        )(*arrays)

    shape = (2, 2, 2, far, half, width)
    block = (2, far, half, width)
    first, first_out, second, second_out = add(
        add_near, [(block, F32), (block, BF16)] * 2, keep.reshape(shape), swap(send.reshape(shape), 1)
    )
    block = (far, half, width)
    first, first_out, second, second_out = add(
        add_next,
        [(block, F32), (block, BF16)] * 2,
        first,
        swap(first_out, 2),
        second,
        swap(second_out, 4),
    )
    block = (tiles, width)
    sums, *parts = add(
        add_far,
        [(block, F32)] + [(block, BF16)] * (far - 1),
        first,
        swap(first_out, 4),
        second,
        swap(second_out, 2),
    )
    parts = [swap(part, s << 3) for s, part in zip(range(1, far), parts)]
    for part in parts:
        sums = sums + part.astype(F32)
    tile_flux = sums / jnp.maximum(counts, 1.0)

    part = guest_rows // 2
    wide = pl.BlockSpec((part, width), lambda i: (i, 0))
    new_state = pl.pallas_call(
        finish_kernel,
        out_shape=jax.ShapeDtypeStruct((capacity, width), F32),
        grid=(-(-capacity // part),),
        in_specs=[SMEM] * 2
        + [wide, wide, pl.BlockSpec((part, width), lambda i: (jnp.minimum(i, 1), 0))],
        out_specs=wide,
        cost_estimate=cost(4.0),
        compiler_params=small,
        name="finish",
    )(owner_counts, other_count, land_state, tend, back)
    return (new_state, tile_flux)


def solution(mesh):
    devices = mesh.shape["atm"] * mesh.shape["land"]
    rows, whole = P(AXES, None), P()

    def body(*arrays):
        return local(devices, *arrays)

    return jax.shard_map(
        body,
        mesh=mesh,
        in_specs=(rows, P(AXES), whole, P(AXES), P(AXES), P(AXES), rows) + (whole,) * 5,
        out_specs=(rows, rows),
        check_vma=False,
    )
```

```python
import functools

import jax
import jax.numpy as jnp
from jax import lax
from jax.experimental import pallas as pl
from jax.experimental.pallas import tpu as pltpu
from jax.sharding import PartitionSpec as P


AXES = ("atm", "land")
ROWS = 256
FIELDS = 8
VMEM = pl.BlockSpec(memory_space=pltpu.VMEM)
SMEM = pl.BlockSpec(memory_space=pltpu.SMEM)
HBM = pl.BlockSpec(memory_space=pltpu.HBM)
BF16 = jnp.bfloat16
F32 = jnp.float32


def iota(shape, dim):
    return lax.broadcasted_iota(jnp.int32, shape, dim)


def dot_nt(a, b):
    return lax.dot_general(a, b, (((1,), (1,)), ((), ())), preferred_element_type=F32)


def hbm(array):
    return pltpu.with_memory_space_constraint(array, pltpu.HBM)


def vmem(array):
    return pltpu.with_memory_space_constraint(array, pltpu.VMEM)


def cost(microseconds):
    return pl.CostEstimate(
        flops=int(microseconds * 8e6), bytes_accessed=int(microseconds * 2e6), transcendentals=0
    )


def bucket_kernel(
    devices,
    capacity,
    tgt_hbm,
    tile_hbm,
    gap_hbm,
    forcing_hbm,
    out_ref,
    count_ref,
    first_ref,
    second_ref,
    tgt_ref,
    tile_ref,
    gap_ref,
    sems,
):
    half = first_ref.shape[0]
    pairs = (
        (tgt_hbm, tgt_ref),
        (tile_hbm, tile_ref),
        (gap_hbm, gap_ref),
        (forcing_hbm.at[pl.ds(0, half)], first_ref),
        (forcing_hbm.at[pl.ds(half, half)], second_ref),
    )
    copies = [pltpu.make_async_copy(*pair, sems.at[place]) for place, pair in enumerate(pairs)]
    for copy in copies:
        copy.start()
    for copy in copies:
        copy.wait()
    columns = tgt_ref.shape[1]
    places = out_ref.shape[1]
    tiles = count_ref.shape[0]
    target = tgt_ref[...]
    peer = jnp.floor((target.astype(F32) + 0.5) * (1.0 / capacity)).astype(jnp.int32)
    slot = target - peer * capacity
    high, low = lax.shift_right_logical(slot, 8), slot & (ROWS - 1)
    tile = tile_ref[...]
    gap = gap_ref[...]
    gap1 = gap.astype(BF16).astype(F32)
    gap2 = (gap - gap1).astype(BF16).astype(F32)
    gap3 = gap - gap1 - gap2
    hot = iota((devices, columns), 0) == peer
    hot_f = jnp.where(hot, 1.0, 0.0)
    hot_b = hot_f.astype(BF16)
    block = min(256, columns)
    upper = jnp.where(iota((block, block), 0) <= iota((block, block), 1), 1.0, 0.0).astype(BF16)
    carry = jnp.zeros((devices, 1), F32)
    ranks = []
    for start in range(0, columns, block):
        part = hot_b[:, start : start + block]
        inside = jnp.dot(part, upper, preferred_element_type=F32)
        here = inside + carry
        ranks.append(jnp.sum(here * hot_f[:, start : start + block], axis=0, keepdims=True))
        carry = carry + inside[:, block - 1 : block]
    rank = jnp.concatenate(ranks, axis=1).astype(jnp.int32) - 1
    place_hot = jnp.where(iota((places, columns), 0) == rank, 1.0, 0.0).astype(BF16)
    zero = jnp.zeros((1, columns), F32)
    fields = jnp.concatenate(
        [
            high.astype(F32) + 1.0,
            low.astype(F32),
            tile.astype(F32),
            gap1,
            gap2,
            gap3,
            zero,
            zero,
        ],
        axis=0,
    )
    spread = jnp.concatenate(
        [jnp.where(peer == device, fields, 0.0) for device in range(devices)], axis=0
    ).astype(BF16)
    out_ref[...] = dot_nt(spread, place_hot).astype(BF16)
    tile_hot = jnp.where(iota((tiles, columns), 0) == tile, 1.0, 0.0).astype(BF16)
    count_ref[...] = jnp.dot(
        tile_hot, jnp.ones((columns, count_ref.shape[1]), BF16), preferred_element_type=F32
    )


def arrange_kernel(devices, tiles, me_ref, got_ref, weight_hbms, mine_ref, guest_ref, weight_refs, sems):
    pairs = zip(weight_hbms, weight_refs)
    copies = [pltpu.make_async_copy(*pair, sems.at[place]) for place, pair in enumerate(pairs)]
    for copy in copies:
        copy.start()
    places = got_ref.shape[1]
    rows = mine_ref.shape[1]
    total = jnp.zeros((5 * rows, ROWS), F32)
    row_id = iota((rows, places), 0).astype(F32) + 1.0
    low_id = iota((ROWS, places), 0).astype(F32)
    for device in range(devices):
        got = got_ref[device * FIELDS : (device + 1) * FIELDS, :].astype(F32)
        hot = got[0:1] == row_id
        zero = jnp.zeros((rows, places), F32)
        parts = [jnp.where(hot, float(device + 1), zero)]
        parts += [jnp.where(hot, got[field : field + 1], zero) for field in (2, 3, 4, 5)]
        left = jnp.concatenate(parts, axis=0).astype(BF16)
        right = jnp.where(low_id == got[1:2], 1.0, 0.0).astype(BF16)
        total = total + dot_nt(left, right)
    source = total[0:rows].astype(jnp.int32) - 1
    tile = total[rows : 2 * rows].astype(jnp.int32)
    gap = total[2 * rows : 3 * rows] + total[3 * rows : 4 * rows] + total[4 * rows :]
    for out_ref, me in ((mine_ref, me_ref[0]), (guest_ref, me_ref[0] ^ 1)):
        row = table_row(devices, tiles, source ^ me, tile)
        out_ref[0] = jnp.where(source >= 0, row, devices * tiles).astype(F32)
        out_ref[1] = gap
    for copy in copies:
        copy.wait()


def table_row(devices, tiles, relative, tile):
    groups, half = devices // 2, tiles // 2
    far = groups // 4
    group = (lax.shift_right_logical(relative, 1) & 3) * far + lax.shift_right_logical(relative, 3)
    part = jnp.where(tile >= half, 1, 0)
    return (relative & 1) * (groups * tiles) + part * (groups * half) + group * half + (tile - part * half)


def tile_ranges(own, other):
    have = (own + (ROWS - 1)) // ROWS
    return jnp.maximum(own - other, 0) // (2 * ROWS), have


def network_kernel(
    own_ref,
    other_ref,
    state_ref,
    guest_ref,
    mine_ref,
    guest_mine_ref,
    even_refs,
    odd_refs,
    lapse_ref,
    gains_ref,
    w_in_ref,
    w_up_ref,
    w_down_ref,
    w_out_ref,
    tend_ref,
    guest_tend_ref,
    keep_ref,
    send_ref,
    table_ref,
    bank_refs,
    rows_ref,
    flux_ref,
    x_ref,
    gap_ref,
    index_ref,
    scalar_ref,
    out_ref,
    h_ref,
    sem,
    out_sems,
):
    half, width = keep_ref.shape
    spare = 2 * half
    given, have = tile_ranges(own_ref[0], other_ref[0])
    taken, _ = tile_ranges(other_ref[0], own_ref[0])
    own_tiles = have - given
    all_tiles = own_tiles + taken
    lines = mine_ref.shape[1]
    last_line = 2 * lines
    guest_rows = guest_tend_ref.shape[0] - ROWS
    lanes = index_ref.shape[1]
    parts = ROWS // lanes
    part_lines = last_line + 8

    for part in range(parts):
        side = slice(part * lanes, (part + 1) * lanes)
        base = part * part_lines
        index_ref[base : base + lines, :] = mine_ref[0, :, side].astype(jnp.int32)
        index_ref[base + lines : base + last_line, :] = guest_mine_ref[0, :, side].astype(jnp.int32)
        index_ref[base + last_line : base + part_lines, :] = jnp.full((8, lanes), spare, jnp.int32)
    copy = pltpu.make_async_copy(index_ref, scalar_ref, sem)
    copy.start()
    for core, pieces in enumerate((even_refs, odd_refs)):
        base = core * half
        run = pieces[0].shape[1] * pieces[0].shape[2]
        for part, piece in enumerate(pieces):
            for other in range(2):
                y, x = (part % 2, other) if part < 2 else (other, part % 2)
                at = base + (part // 2) * (half // 2) + (2 * y + x) * run
                table_ref[at : at + run, :] = piece[other].astype(F32).reshape(run, width)
    table_ref[spare:, :] = jnp.zeros_like(table_ref[spare:, :])
    for bank in bank_refs:
        bank[...] = jnp.zeros_like(bank)
    copy.wait()

    def norm(values, gain):
        scale = lax.rsqrt(jnp.mean(values * values, axis=-1, keepdims=True) + 1e-06)
        return (values * scale * gain).astype(BF16)

    def place_of(step):
        is_own = step < own_tiles
        index = jnp.where(is_own, step + given, step - own_tiles)
        index = jnp.where(step < all_tiles, index, 0)
        return is_own, index, pl.multiple_of(index * ROWS, ROWS)

    def line_of(step):
        is_own, index, _ = place_of(step)
        line = jnp.where(is_own, index, index + lines)
        return jnp.where((step >= 0) & (step < all_tiles), line, last_line)

    def fetch(step):
        for chain in range(2):
            line = line_of(2 * step + chain)
            for row in range(ROWS):
                at = chain * ROWS + row
                where = scalar_ref[line + row // lanes * part_lines, row % lanes]
                rows_ref[at : at + 1, :] = table_ref[pl.ds(where, 1), :]

    def spread(step):
        for chain in range(2):
            line = line_of(2 * step + chain)
            for row in range(ROWS):
                at = chain * ROWS + row
                bank = bank_refs[row % len(bank_refs)]
                where = pl.ds(scalar_ref[line + row // lanes * part_lines, row % lanes], 1)
                bank[where, :] = bank[where, :] + flux_ref[at : at + 1, :]

    def load(chain, step):
        is_own, index, start = place_of(step)

        @pl.when(is_own)
        def _():
            x_ref[chain] = state_ref[pl.ds(start, ROWS), :].astype(BF16)
            gap_ref[chain] = jnp.broadcast_to(mine_ref[1, pl.ds(index, 1), :], (8, ROWS))

        @pl.when(jnp.logical_not(is_own))
        def _():
            x_ref[chain] = guest_ref[pl.ds(start, ROWS), :].astype(BF16)
            gap_ref[chain] = jnp.broadcast_to(guest_mine_ref[1, pl.ds(index, 1), :], (8, ROWS))

    def store(chain, step, tend):
        is_own, _, start = place_of(step)
        start = pl.multiple_of(jnp.where(step < all_tiles, start, guest_rows), ROWS)

        @pl.when(step >= 2)
        def _():
            arrived(chain)

        out_ref[chain] = tend

        @pl.when(is_own)
        def _():
            pltpu.make_async_copy(
                out_ref.at[chain], tend_ref.at[pl.ds(start, ROWS)], out_sems.at[chain]
            ).start()

        @pl.when(jnp.logical_not(is_own))
        def _():
            pltpu.make_async_copy(
                out_ref.at[chain], guest_tend_ref.at[pl.ds(start, ROWS)], out_sems.at[chain]
            ).start()

    def arrived(chain):
        pltpu.make_async_copy(
            out_ref.at[chain], tend_ref.at[pl.ds(0, ROWS)], out_sems.at[chain]
        ).wait()

    chains = range(2)

    def load_pair(step):
        for chain in chains:
            load(chain, 2 * step + chain)

    def enter(chain):
        gap = jnp.transpose(gap_ref[chain])[:, 0:1]
        forcing = rows_ref[chain * ROWS : (chain + 1) * ROWS, :] + gap * lapse_ref[...]
        inputs = jnp.concatenate([forcing.astype(BF16), x_ref[chain]], axis=1)
        h_ref[chain] = jnp.dot(inputs, w_in_ref[...], preferred_element_type=F32)

    def two_tiles(step, _):
        load_pair(step + 1)
        spread(step - 1)
        low = [norm(h_ref[chain], gains_ref[0:1, :]) for chain in chains]
        up = [jnp.dot(v, w_up_ref[...], preferred_element_type=F32) for v in low]
        active = [(v * (0.5 + 0.5 * jnp.tanh(0.5 * v))).astype(BF16) for v in up]
        h = [
            h_ref[chain] + jnp.dot(active[chain], w_down_ref[...], preferred_element_type=F32)
            for chain in chains
        ]
        for chain in chains:
            enter(chain)
        fetch(step + 2)
        low = [norm(v, gains_ref[1:2, :]) for v in h]
        result = [jnp.dot(v, w_out_ref[...], preferred_element_type=F32) for v in low]
        for chain in chains:
            flux_ref[chain * ROWS : (chain + 1) * ROWS, :] = (
                result[chain][:, width:].astype(BF16).astype(F32)
            )
        for chain in chains:
            store(chain, 2 * step + chain, result[chain][:, :width].astype(BF16))
        return 0

    steps = (all_tiles + 1) // 2
    fetch(0)
    load_pair(0)
    for chain in chains:
        enter(chain)
    fetch(1)
    lax.fori_loop(0, steps, two_tiles, 0)
    spread(steps - 1)
    chunk = min(half, 128)

    def gather(place, _):
        low = pl.ds(pl.multiple_of(place * chunk, chunk), chunk)
        high = pl.ds(pl.multiple_of(half + place * chunk, chunk), chunk)
        keep_ref[low, :] = functools.reduce(jnp.add, [bank[low, :] for bank in bank_refs])
        sums = functools.reduce(jnp.add, [bank[high, :] for bank in bank_refs])
        send_ref[low, :] = sums.astype(BF16)
        return 0

    lax.fori_loop(0, half // chunk, gather, 0)
    for chain in range(2):
        arrived(chain)


def finish_kernel(own_ref, other_ref, state_ref, tend_ref, back_ref, out_ref):
    own = own_ref[0]
    given, _ = tile_ranges(own, other_ref[0])
    rows = out_ref.shape[0]
    slot = iota((rows, 1), 0) + pl.program_id(0) * rows
    change = jnp.where(slot < given * ROWS, back_ref[...].astype(F32), tend_ref[...].astype(F32))
    out_ref[...] = jnp.where(slot < own, state_ref[...] + change, 0.0)


def add_near(keep_ref, in_ref, first_ref, first_out_ref, second_ref, second_out_ref):
    for other in range(2):
        first_ref[other] = keep_ref[0, other, 0] + in_ref[0, other, 0].astype(F32)
        second_ref[other] = keep_ref[1, 0, other] + in_ref[1, 0, other].astype(F32)
        first_out_ref[other] = (keep_ref[0, other, 1] + in_ref[0, other, 1].astype(F32)).astype(BF16)
        second_out_ref[other] = (keep_ref[1, 1, other] + in_ref[1, 1, other].astype(F32)).astype(BF16)


def add_next(a_ref, a_in_ref, b_ref, b_in_ref, first_ref, first_out_ref, second_ref, second_out_ref):
    first_ref[...] = a_ref[0] + a_in_ref[0].astype(F32)
    second_ref[...] = b_ref[0] + b_in_ref[0].astype(F32)
    first_out_ref[...] = (a_ref[1] + a_in_ref[1].astype(F32)).astype(BF16)
    second_out_ref[...] = (b_ref[1] + b_in_ref[1].astype(F32)).astype(BF16)


def add_far(a_ref, a_in_ref, b_ref, b_in_ref, sum_ref, *out_refs):
    half = a_ref.shape[1]
    for far, out_ref in enumerate((sum_ref,) + out_refs):
        out_ref[0:half, :] = (a_ref[far] + a_in_ref[far].astype(F32)).astype(out_ref.dtype)
        out_ref[half:, :] = (b_ref[far] + b_in_ref[far].astype(F32)).astype(out_ref.dtype)


def local(
    devices,
    tile_forcing,
    elevation_gap,
    lapse_rate,
    column_tile,
    column_target,
    owner_counts,
    land_state,
    w_in,
    norm_gains,
    w_up,
    w_down,
    w_out,
):
    capacity, width = land_state.shape
    per_peer = capacity // devices + 1
    places = -(-per_peer // 128) * 128
    columns = elevation_gap.shape[0]
    tiles = tile_forcing.shape[0]
    guest_rows = -(-capacity // (2 * ROWS)) * ROWS
    meta_rows = -(-capacity // (8 * ROWS)) * 8
    bits = devices.bit_length() - 1
    me = lax.axis_index(AXES)

    def swap(values, bit):
        return lax.ppermute(values, AXES, [(i, i ^ bit) for i in range(devices)])

    small = pltpu.CompilerParams(vmem_limit_bytes=24 << 20)
    half = tiles // 2
    buckets, counts, own_first, own_second = pl.pallas_call(
        functools.partial(bucket_kernel, devices, capacity),
        out_shape=(
            jax.ShapeDtypeStruct((devices * FIELDS, places), BF16),
            jax.ShapeDtypeStruct((tiles, width), F32),
            jax.ShapeDtypeStruct((half, width), BF16),
            jax.ShapeDtypeStruct((half, width), BF16),
        ),
        in_specs=[HBM] * 4,
        out_specs=(VMEM,) * 4,
        scratch_shapes=[
            pltpu.VMEM((1, columns), jnp.int32),
            pltpu.VMEM((1, columns), jnp.int32),
            pltpu.VMEM((1, columns), F32),
            pltpu.SemaphoreType.DMA((5,)),
        ],
        cost_estimate=cost(3.0),
        compiler_params=small,
        name="bucket",
    )(
        hbm(column_target.reshape(1, columns)),
        hbm(column_tile.reshape(1, columns)),
        hbm(elevation_gap.reshape(1, columns)),
        hbm(tile_forcing),
    )
    got = lax.all_to_all(
        buckets.reshape(devices, FIELDS, places), AXES, split_axis=0, concat_axis=0, tiled=True
    )
    far = 1 << (bits - 3)
    gathered = []
    for s in range(1, far):
        gathered.append(swap(tile_forcing, s << 3))
    first = jnp.stack([own_first] + [piece[:half] for piece in gathered])
    second = jnp.stack([own_second] + [piece[half:] for piece in gathered])
    first = jnp.stack([first, swap(first, 2)])
    second = jnp.stack([second, swap(second, 4)])
    even = (first, swap(first, 4), second, swap(second, 2))
    groups = devices // 2
    odd = tuple(swap(piece, 1) for piece in even)

    other_count = swap(owner_counts, 1)
    guest_state = swap(land_state, 1)

    weights = (w_in, w_up[0], w_down[0], w_out)
    mine, theirs, weights = pl.pallas_call(
        functools.partial(arrange_kernel, devices, tiles),
        out_shape=(jax.ShapeDtypeStruct((2, meta_rows, ROWS), F32),) * 2
        + (tuple(jax.ShapeDtypeStruct(w.shape, BF16) for w in weights),),
        in_specs=[SMEM, VMEM, (HBM,) * 4],
        out_specs=(VMEM, VMEM, (VMEM,) * 4),
        scratch_shapes=[pltpu.SemaphoreType.DMA((4,))],
        cost_estimate=cost(4.0),
        compiler_params=small,
        name="arrange",
    )(
        me.astype(jnp.int32)[None],
        got.reshape(devices * FIELDS, places),
        tuple(hbm(w) for w in weights),
    )
    guest_mine = swap(theirs, 1)
    table_rows = devices * tiles
    held = vmem if table_rows <= 8192 else hbm
    network_bytes = (
        (14 << 20)
        + capacity * width * 12
        + table_rows * width * (4 * (5 if table_rows <= 8192 else 2) + 10)
    )
    if table_rows > 8192:
        network_bytes = 60 * 1024 * 1024
    tend, guest_tend, keep, send = pl.pallas_call(
        network_kernel,
        out_shape=(
            jax.ShapeDtypeStruct((capacity, width), BF16),
            jax.ShapeDtypeStruct((guest_rows + ROWS, width), BF16),
            jax.ShapeDtypeStruct((groups * tiles, width), F32),
            jax.ShapeDtypeStruct((groups * tiles, width), BF16),
        ),
        in_specs=[SMEM] * 2 + [VMEM] * 4 + [(VMEM,) * 4] * 2 + [VMEM] * 6,
        out_specs=(HBM, HBM, VMEM, VMEM),
        scratch_shapes=[
            pltpu.VMEM((table_rows + 8, width), F32),
            [pltpu.VMEM((table_rows + 8, width), F32)] * (4 if table_rows <= 8192 else 1),
            pltpu.VMEM((2 * ROWS, width), F32),
            pltpu.VMEM((2 * ROWS, width), F32),
            pltpu.VMEM((2, ROWS, width), BF16),
            pltpu.VMEM((2, 8, ROWS), F32),
            pltpu.VMEM((ROWS // width * (2 * meta_rows + 8), width), jnp.int32),
            pltpu.SMEM((ROWS // width * (2 * meta_rows + 8), width), jnp.int32),
            pltpu.VMEM((2, ROWS, width), BF16),
            pltpu.VMEM((2, ROWS, w_in.shape[1]), F32),
            pltpu.SemaphoreType.DMA,
            pltpu.SemaphoreType.DMA((2,)),
        ],
        cost_estimate=cost(50.0),
        compiler_params=pltpu.CompilerParams(vmem_limit_bytes=network_bytes),
        name="network",
    )(
        owner_counts,
        other_count,
        land_state,
        held(guest_state),
        mine,
        guest_mine,
        tuple(held(piece) for piece in even),
        tuple(held(piece) for piece in odd),
        lapse_rate.reshape(1, width),
        norm_gains,
        *(held(w) for w in weights),
    )
    back = swap(guest_tend, 1)

    def add(kernel, shapes, *arrays):
        return pl.pallas_call(
            kernel,
            out_shape=tuple(jax.ShapeDtypeStruct(shape, dtype) for shape, dtype in shapes),
            in_specs=[VMEM] * len(arrays),
            out_specs=(VMEM,) * len(shapes),
            cost_estimate=cost(0.5),
            compiler_params=small,
            name="add",
        )(*arrays)

    shape = (2, 2, 2, far, half, width)
    block = (2, far, half, width)
    first, first_out, second, second_out = add(
        add_near, [(block, F32), (block, BF16)] * 2, keep.reshape(shape), swap(send.reshape(shape), 1)
    )
    block = (far, half, width)
    first, first_out, second, second_out = add(
        add_next,
        [(block, F32), (block, BF16)] * 2,
        first,
        swap(first_out, 2),
        second,
        swap(second_out, 4),
    )
    block = (tiles, width)
    sums, *parts = add(
        add_far,
        [(block, F32)] + [(block, BF16)] * (far - 1),
        first,
        swap(first_out, 4),
        second,
        swap(second_out, 2),
    )
    here = []
    for s, part in zip(range(1, far), parts):
        here.append(swap(part, s << 3))
    parts = here
    for part in parts:
        sums = sums + part.astype(F32)
    tile_flux = sums / jnp.maximum(counts, 1.0)

    part = guest_rows // 2
    wide = pl.BlockSpec((part, width), lambda i: (i, 0))
    new_state = pl.pallas_call(
        finish_kernel,
        out_shape=jax.ShapeDtypeStruct((capacity, width), F32),
        grid=(-(-capacity // part),),
        in_specs=[SMEM] * 2
        + [wide, wide, pl.BlockSpec((part, width), lambda i: (jnp.minimum(i, 1), 0))],
        out_specs=wide,
        cost_estimate=cost(4.0),
        compiler_params=small,
        name="finish",
    )(owner_counts, other_count, land_state, tend, back)
    return (new_state, tile_flux)


def solution(mesh):
    devices = mesh.shape["atm"] * mesh.shape["land"]
    rows, whole = P(AXES, None), P()

    def body(*arrays):
        return local(devices, *arrays)

    return jax.shard_map(
        body,
        mesh=mesh,
        in_specs=(rows, P(AXES), whole, P(AXES), P(AXES), P(AXES), rows) + (whole,) * 5,
        out_specs=(rows, rows),
        check_vma=False,
    )
```

```python
import functools

import jax
import jax.numpy as jnp
from jax import lax
from jax.experimental import pallas as pl
from jax.experimental.pallas import tpu as pltpu
from jax.sharding import PartitionSpec as P


AXES = ("atm", "land")
ROWS = 256
FIELDS = 8
VMEM = pl.BlockSpec(memory_space=pltpu.VMEM)
SMEM = pl.BlockSpec(memory_space=pltpu.SMEM)
HBM = pl.BlockSpec(memory_space=pltpu.HBM)
BF16 = jnp.bfloat16
F32 = jnp.float32


def iota(shape, dim):
    return lax.broadcasted_iota(jnp.int32, shape, dim)


def dot_nt(a, b):
    return lax.dot_general(a, b, (((1,), (1,)), ((), ())), preferred_element_type=F32)


def hbm(array):
    return pltpu.with_memory_space_constraint(array, pltpu.HBM)


def vmem(array):
    return pltpu.with_memory_space_constraint(array, pltpu.VMEM)


def cost(microseconds):
    return pl.CostEstimate(
        flops=int(microseconds * 8e6), bytes_accessed=int(microseconds * 2e6), transcendentals=0
    )


def bucket_kernel(
    devices,
    capacity,
    tgt_hbm,
    tile_hbm,
    gap_hbm,
    forcing_hbm,
    out_ref,
    first_ref,
    second_ref,
    tgt_ref,
    tile_ref,
    gap_ref,
    sems,
):
    half = first_ref.shape[0]
    pairs = (
        (tgt_hbm, tgt_ref),
        (tile_hbm, tile_ref),
        (gap_hbm, gap_ref),
        (forcing_hbm.at[pl.ds(0, half)], first_ref),
        (forcing_hbm.at[pl.ds(half, half)], second_ref),
    )
    copies = [pltpu.make_async_copy(*pair, sems.at[place]) for place, pair in enumerate(pairs)]
    for copy in copies:
        copy.start()
    for copy in copies:
        copy.wait()
    columns = tgt_ref.shape[1]
    places = out_ref.shape[1]
    target = tgt_ref[...]
    peer = jnp.floor((target.astype(F32) + 0.5) * (1.0 / capacity)).astype(jnp.int32)
    slot = target - peer * capacity
    high, low = lax.shift_right_logical(slot, 8), slot & (ROWS - 1)
    tile = tile_ref[...]
    gap = gap_ref[...]
    gap1 = gap.astype(BF16).astype(F32)
    gap2 = (gap - gap1).astype(BF16).astype(F32)
    gap3 = gap - gap1 - gap2
    hot = iota((devices, columns), 0) == peer
    hot_f = jnp.where(hot, 1.0, 0.0)
    hot_b = hot_f.astype(BF16)
    block = min(256, columns)
    upper = jnp.where(iota((block, block), 0) <= iota((block, block), 1), 1.0, 0.0).astype(BF16)
    carry = jnp.zeros((devices, 1), F32)
    ranks = []
    for start in range(0, columns, block):
        part = hot_b[:, start : start + block]
        inside = jnp.dot(part, upper, preferred_element_type=F32)
        here = inside + carry
        ranks.append(jnp.sum(here * hot_f[:, start : start + block], axis=0, keepdims=True))
        carry = carry + inside[:, block - 1 : block]
    rank = jnp.concatenate(ranks, axis=1).astype(jnp.int32) - 1
    place_hot = jnp.where(iota((places, columns), 0) == rank, 1.0, 0.0).astype(BF16)
    zero = jnp.zeros((1, columns), F32)
    fields = jnp.concatenate(
        [
            high.astype(F32) + 1.0,
            low.astype(F32),
            tile.astype(F32),
            gap1,
            gap2,
            gap3,
            zero,
            zero,
        ],
        axis=0,
    )
    spread = jnp.concatenate(
        [jnp.where(peer == device, fields, 0.0) for device in range(devices)], axis=0
    ).astype(BF16)
    out_ref[...] = dot_nt(spread, place_hot).astype(BF16)


def arrange_kernel(devices, tiles, me_ref, got_ref, weight_hbms, mine_ref, guest_ref, weight_refs, sems):
    pairs = zip(weight_hbms, weight_refs)
    copies = [pltpu.make_async_copy(*pair, sems.at[place]) for place, pair in enumerate(pairs)]
    for copy in copies:
        copy.start()
    places = got_ref.shape[1]
    rows = mine_ref.shape[1]
    total = jnp.zeros((5 * rows, ROWS), F32)
    row_id = iota((rows, places), 0).astype(F32) + 1.0
    low_id = iota((ROWS, places), 0).astype(F32)
    for device in range(devices):
        got = got_ref[device * FIELDS : (device + 1) * FIELDS, :].astype(F32)
        hot = got[0:1] == row_id
        zero = jnp.zeros((rows, places), F32)
        parts = [jnp.where(hot, float(device + 1), zero)]
        parts += [jnp.where(hot, got[field : field + 1], zero) for field in (2, 3, 4, 5)]
        left = jnp.concatenate(parts, axis=0).astype(BF16)
        right = jnp.where(low_id == got[1:2], 1.0, 0.0).astype(BF16)
        total = total + dot_nt(left, right)
    source = total[0:rows].astype(jnp.int32) - 1
    tile = total[rows : 2 * rows].astype(jnp.int32)
    gap = total[2 * rows : 3 * rows] + total[3 * rows : 4 * rows] + total[4 * rows :]
    for out_ref, me in ((mine_ref, me_ref[0]), (guest_ref, me_ref[0] ^ 1)):
        row = table_row(devices, tiles, source ^ me, tile)
        out_ref[0] = jnp.where(source >= 0, row, devices * tiles).astype(F32)
        out_ref[1] = gap
    for copy in copies:
        copy.wait()


def table_row(devices, tiles, relative, tile):
    groups, half = devices // 2, tiles // 2
    far = groups // 4
    group = (lax.shift_right_logical(relative, 1) & 3) * far + lax.shift_right_logical(relative, 3)
    part = jnp.where(tile >= half, 1, 0)
    return (relative & 1) * (groups * tiles) + part * (groups * half) + group * half + (tile - part * half)


def tile_ranges(own, other):
    have = (own + (ROWS - 1)) // ROWS
    return jnp.maximum(own - other, 0) // (2 * ROWS), have


def network_kernel(
    own_ref,
    other_ref,
    state_ref,
    guest_ref,
    mine_ref,
    guest_mine_ref,
    even_refs,
    odd_refs,
    lapse_ref,
    gains_ref,
    w_in_ref,
    w_up_ref,
    w_down_ref,
    w_out_ref,
    tend_ref,
    guest_tend_ref,
    keep_ref,
    send_ref,
    table_ref,
    bank_refs,
    rows_ref,
    flux_ref,
    x_ref,
    gap_ref,
    index_ref,
    scalar_ref,
    out_ref,
    h_ref,
    sem,
    out_sems,
):
    half, width = keep_ref.shape
    spare = 2 * half
    given, have = tile_ranges(own_ref[0], other_ref[0])
    taken, _ = tile_ranges(other_ref[0], own_ref[0])
    own_tiles = have - given
    all_tiles = own_tiles + taken
    lines = mine_ref.shape[1]
    last_line = 2 * lines
    guest_rows = guest_tend_ref.shape[0] - ROWS
    lanes = index_ref.shape[1]
    parts = ROWS // lanes
    part_lines = last_line + 8

    for part in range(parts):
        side = slice(part * lanes, (part + 1) * lanes)
        base = part * part_lines
        index_ref[base : base + lines, :] = mine_ref[0, :, side].astype(jnp.int32)
        index_ref[base + lines : base + last_line, :] = guest_mine_ref[0, :, side].astype(jnp.int32)
        index_ref[base + last_line : base + part_lines, :] = jnp.full((8, lanes), spare, jnp.int32)
    copy = pltpu.make_async_copy(index_ref, scalar_ref, sem)
    copy.start()
    for core, pieces in enumerate((even_refs, odd_refs)):
        base = core * half
        run = pieces[0].shape[1] * pieces[0].shape[2]
        for part, piece in enumerate(pieces):
            for other in range(2):
                y, x = (part % 2, other) if part < 2 else (other, part % 2)
                at = base + (part // 2) * (half // 2) + (2 * y + x) * run
                table_ref[at : at + run, :] = piece[other].astype(F32).reshape(run, width)
    table_ref[spare:, :] = jnp.zeros_like(table_ref[spare:, :])
    for bank in bank_refs:
        bank[...] = jnp.zeros_like(bank)
    copy.wait()

    def norm(values, gain):
        scale = lax.rsqrt(jnp.mean(values * values, axis=-1, keepdims=True) + 1e-06)
        return (values * scale * gain).astype(BF16)

    def place_of(step):
        is_own = step < own_tiles
        index = jnp.where(is_own, step + given, step - own_tiles)
        index = jnp.where(step < all_tiles, index, 0)
        return is_own, index, pl.multiple_of(index * ROWS, ROWS)

    def line_of(step):
        is_own, index, _ = place_of(step)
        line = jnp.where(is_own, index, index + lines)
        return jnp.where((step >= 0) & (step < all_tiles), line, last_line)

    def fetch(step):
        for chain in range(2):
            line = line_of(2 * step + chain)
            for row in range(ROWS):
                at = chain * ROWS + row
                where = scalar_ref[line + row // lanes * part_lines, row % lanes]
                rows_ref[at : at + 1, :] = table_ref[pl.ds(where, 1), :]

    def spread(step):
        for chain in range(2):
            line = line_of(2 * step + chain)
            for row in range(ROWS):
                at = chain * ROWS + row
                bank = bank_refs[row % len(bank_refs)]
                where = pl.ds(scalar_ref[line + row // lanes * part_lines, row % lanes], 1)
                bank[where, :] = bank[where, :] + flux_ref[at : at + 1, :]

    def load(chain, step):
        is_own, index, start = place_of(step)

        @pl.when(is_own)
        def _():
            x_ref[chain] = state_ref[pl.ds(start, ROWS), :].astype(BF16)
            gap_ref[chain] = jnp.broadcast_to(mine_ref[1, pl.ds(index, 1), :], (8, ROWS))

        @pl.when(jnp.logical_not(is_own))
        def _():
            x_ref[chain] = guest_ref[pl.ds(start, ROWS), :].astype(BF16)
            gap_ref[chain] = jnp.broadcast_to(guest_mine_ref[1, pl.ds(index, 1), :], (8, ROWS))

    def store(chain, step, tend):
        is_own, _, start = place_of(step)
        start = pl.multiple_of(jnp.where(step < all_tiles, start, guest_rows), ROWS)

        @pl.when(step >= 2)
        def _():
            arrived(chain)

        out_ref[chain] = tend

        @pl.when(is_own)
        def _():
            pltpu.make_async_copy(
                out_ref.at[chain], tend_ref.at[pl.ds(start, ROWS)], out_sems.at[chain]
            ).start()

        @pl.when(jnp.logical_not(is_own))
        def _():
            pltpu.make_async_copy(
                out_ref.at[chain], guest_tend_ref.at[pl.ds(start, ROWS)], out_sems.at[chain]
            ).start()

    def arrived(chain):
        pltpu.make_async_copy(
            out_ref.at[chain], tend_ref.at[pl.ds(0, ROWS)], out_sems.at[chain]
        ).wait()

    chains = range(2)

    def load_pair(step):
        for chain in chains:
            load(chain, 2 * step + chain)

    def enter(chain):
        gap = jnp.transpose(gap_ref[chain])[:, 0:1]
        forcing = rows_ref[chain * ROWS : (chain + 1) * ROWS, :] + gap * lapse_ref[...]
        inputs = jnp.concatenate([forcing.astype(BF16), x_ref[chain]], axis=1)
        h_ref[chain] = jnp.dot(inputs, w_in_ref[...], preferred_element_type=F32)

    def two_tiles(step, _):
        load_pair(step + 1)
        spread(step - 1)
        low = [norm(h_ref[chain], gains_ref[0:1, :]) for chain in chains]
        up = [jnp.dot(v, w_up_ref[...], preferred_element_type=F32) for v in low]
        active = [(v * (0.5 + 0.5 * jnp.tanh(0.5 * v))).astype(BF16) for v in up]
        h = [
            h_ref[chain] + jnp.dot(active[chain], w_down_ref[...], preferred_element_type=F32)
            for chain in chains
        ]
        for chain in chains:
            enter(chain)
        fetch(step + 2)
        low = [norm(v, gains_ref[1:2, :]) for v in h]
        result = [jnp.dot(v, w_out_ref[...], preferred_element_type=F32) for v in low]
        for chain in chains:
            flux_ref[chain * ROWS : (chain + 1) * ROWS, :] = (
                result[chain][:, width:].astype(BF16).astype(F32)
            )
        for chain in chains:
            store(chain, 2 * step + chain, result[chain][:, :width].astype(BF16))
        return 0

    steps = (all_tiles + 1) // 2
    fetch(0)
    load_pair(0)
    for chain in chains:
        enter(chain)
    fetch(1)
    lax.fori_loop(0, steps, two_tiles, 0)
    spread(steps - 1)
    chunk = min(half, 128)

    def gather(place, _):
        low = pl.ds(pl.multiple_of(place * chunk, chunk), chunk)
        high = pl.ds(pl.multiple_of(half + place * chunk, chunk), chunk)
        keep_ref[low, :] = functools.reduce(jnp.add, [bank[low, :] for bank in bank_refs])
        sums = functools.reduce(jnp.add, [bank[high, :] for bank in bank_refs])
        send_ref[low, :] = sums.astype(BF16)
        return 0

    lax.fori_loop(0, half // chunk, gather, 0)
    for chain in range(2):
        arrived(chain)


def finish_kernel(own_ref, other_ref, state_ref, tend_ref, back_ref, tile_ref, out_ref, count_ref):
    @pl.when(pl.program_id(0) == 0)
    def _():
        tiles, columns = count_ref.shape[0], tile_ref.shape[1]
        hot = jnp.where(iota((tiles, columns), 0) == tile_ref[...], 1.0, 0.0).astype(BF16)
        ones = jnp.ones((columns, count_ref.shape[1]), BF16)
        count_ref[...] = jnp.dot(hot, ones, preferred_element_type=F32)

    own = own_ref[0]
    given, _ = tile_ranges(own, other_ref[0])
    rows = out_ref.shape[0]
    slot = iota((rows, 1), 0) + pl.program_id(0) * rows
    change = jnp.where(slot < given * ROWS, back_ref[...].astype(F32), tend_ref[...].astype(F32))
    out_ref[...] = jnp.where(slot < own, state_ref[...] + change, 0.0)


def add_near(keep_ref, in_ref, first_ref, first_out_ref, second_ref, second_out_ref):
    for other in range(2):
        first_ref[other] = keep_ref[0, other, 0] + in_ref[0, other, 0].astype(F32)
        second_ref[other] = keep_ref[1, 0, other] + in_ref[1, 0, other].astype(F32)
        first_out_ref[other] = (keep_ref[0, other, 1] + in_ref[0, other, 1].astype(F32)).astype(BF16)
        second_out_ref[other] = (keep_ref[1, 1, other] + in_ref[1, 1, other].astype(F32)).astype(BF16)


def add_next(a_ref, a_in_ref, b_ref, b_in_ref, first_ref, first_out_ref, second_ref, second_out_ref):
    first_ref[...] = a_ref[0] + a_in_ref[0].astype(F32)
    second_ref[...] = b_ref[0] + b_in_ref[0].astype(F32)
    first_out_ref[...] = (a_ref[1] + a_in_ref[1].astype(F32)).astype(BF16)
    second_out_ref[...] = (b_ref[1] + b_in_ref[1].astype(F32)).astype(BF16)


def add_far(a_ref, a_in_ref, b_ref, b_in_ref, sum_ref, *out_refs):
    half = a_ref.shape[1]
    for far, out_ref in enumerate((sum_ref,) + out_refs):
        out_ref[0:half, :] = (a_ref[far] + a_in_ref[far].astype(F32)).astype(out_ref.dtype)
        out_ref[half:, :] = (b_ref[far] + b_in_ref[far].astype(F32)).astype(out_ref.dtype)


def local(
    devices,
    tile_forcing,
    elevation_gap,
    lapse_rate,
    column_tile,
    column_target,
    owner_counts,
    land_state,
    w_in,
    norm_gains,
    w_up,
    w_down,
    w_out,
):
    capacity, width = land_state.shape
    per_peer = capacity // devices + 1
    places = -(-per_peer // 128) * 128
    columns = elevation_gap.shape[0]
    tiles = tile_forcing.shape[0]
    guest_rows = -(-capacity // (2 * ROWS)) * ROWS
    meta_rows = -(-capacity // (8 * ROWS)) * 8
    bits = devices.bit_length() - 1
    me = lax.axis_index(AXES)

    def swap(values, bit):
        return lax.ppermute(values, AXES, [(i, i ^ bit) for i in range(devices)])

    small = pltpu.CompilerParams(vmem_limit_bytes=24 << 20)
    half = tiles // 2
    buckets, own_first, own_second = pl.pallas_call(
        functools.partial(bucket_kernel, devices, capacity),
        out_shape=(
            jax.ShapeDtypeStruct((devices * FIELDS, places), BF16),
            jax.ShapeDtypeStruct((half, width), BF16),
            jax.ShapeDtypeStruct((half, width), BF16),
        ),
        in_specs=[HBM] * 4,
        out_specs=(VMEM,) * 3,
        scratch_shapes=[
            pltpu.VMEM((1, columns), jnp.int32),
            pltpu.VMEM((1, columns), jnp.int32),
            pltpu.VMEM((1, columns), F32),
            pltpu.SemaphoreType.DMA((5,)),
        ],
        cost_estimate=cost(3.0),
        compiler_params=small,
        name="bucket",
    )(
        hbm(column_target.reshape(1, columns)),
        hbm(column_tile.reshape(1, columns)),
        hbm(elevation_gap.reshape(1, columns)),
        hbm(tile_forcing),
    )
    got = lax.all_to_all(
        buckets.reshape(devices, FIELDS, places), AXES, split_axis=0, concat_axis=0, tiled=True
    )
    far = 1 << (bits - 3)
    gathered = []
    for s in range(1, far):
        gathered.append(swap(tile_forcing, s << 3))
    first = jnp.stack([own_first] + [piece[:half] for piece in gathered])
    second = jnp.stack([own_second] + [piece[half:] for piece in gathered])
    first = jnp.stack([first, swap(first, 2)])
    second = jnp.stack([second, swap(second, 4)])
    even = (first, swap(first, 4), second, swap(second, 2))
    groups = devices // 2
    odd = tuple(swap(piece, 1) for piece in even)

    other_count = swap(owner_counts, 1)
    guest_state = swap(land_state, 1)

    weights = (w_in, w_up[0], w_down[0], w_out)
    mine, theirs, weights = pl.pallas_call(
        functools.partial(arrange_kernel, devices, tiles),
        out_shape=(jax.ShapeDtypeStruct((2, meta_rows, ROWS), F32),) * 2
        + (tuple(jax.ShapeDtypeStruct(w.shape, BF16) for w in weights),),
        in_specs=[SMEM, VMEM, (HBM,) * 4],
        out_specs=(VMEM, VMEM, (VMEM,) * 4),
        scratch_shapes=[pltpu.SemaphoreType.DMA((4,))],
        cost_estimate=cost(4.0),
        compiler_params=small,
        name="arrange",
    )(
        me.astype(jnp.int32)[None],
        got.reshape(devices * FIELDS, places),
        tuple(hbm(w) for w in weights),
    )
    guest_mine = swap(theirs, 1)
    table_rows = devices * tiles
    held = vmem if table_rows <= 8192 else hbm
    network_bytes = (
        (14 << 20)
        + capacity * width * 12
        + table_rows * width * (4 * (5 if table_rows <= 8192 else 2) + 10)
    )
    if table_rows > 8192:
        network_bytes = 60 * 1024 * 1024
    tend, guest_tend, keep, send = pl.pallas_call(
        network_kernel,
        out_shape=(
            jax.ShapeDtypeStruct((capacity, width), BF16),
            jax.ShapeDtypeStruct((guest_rows + ROWS, width), BF16),
            jax.ShapeDtypeStruct((groups * tiles, width), F32),
            jax.ShapeDtypeStruct((groups * tiles, width), BF16),
        ),
        in_specs=[SMEM] * 2 + [VMEM] * 4 + [(VMEM,) * 4] * 2 + [VMEM] * 6,
        out_specs=(HBM, HBM, VMEM, VMEM),
        scratch_shapes=[
            pltpu.VMEM((table_rows + 8, width), F32),
            [pltpu.VMEM((table_rows + 8, width), F32)] * (4 if table_rows <= 8192 else 1),
            pltpu.VMEM((2 * ROWS, width), F32),
            pltpu.VMEM((2 * ROWS, width), F32),
            pltpu.VMEM((2, ROWS, width), BF16),
            pltpu.VMEM((2, 8, ROWS), F32),
            pltpu.VMEM((ROWS // width * (2 * meta_rows + 8), width), jnp.int32),
            pltpu.SMEM((ROWS // width * (2 * meta_rows + 8), width), jnp.int32),
            pltpu.VMEM((2, ROWS, width), BF16),
            pltpu.VMEM((2, ROWS, w_in.shape[1]), F32),
            pltpu.SemaphoreType.DMA,
            pltpu.SemaphoreType.DMA((2,)),
        ],
        cost_estimate=cost(50.0),
        compiler_params=pltpu.CompilerParams(vmem_limit_bytes=network_bytes),
        name="network",
    )(
        owner_counts,
        other_count,
        land_state,
        held(guest_state),
        mine,
        guest_mine,
        tuple(held(piece) for piece in even),
        tuple(held(piece) for piece in odd),
        lapse_rate.reshape(1, width),
        norm_gains,
        *(held(w) for w in weights),
    )
    back = swap(guest_tend, 1)

    def add(kernel, shapes, *arrays):
        return pl.pallas_call(
            kernel,
            out_shape=tuple(jax.ShapeDtypeStruct(shape, dtype) for shape, dtype in shapes),
            in_specs=[VMEM] * len(arrays),
            out_specs=(VMEM,) * len(shapes),
            cost_estimate=cost(0.5),
            compiler_params=small,
            name="add",
        )(*arrays)

    shape = (2, 2, 2, far, half, width)
    block = (2, far, half, width)
    first, first_out, second, second_out = add(
        add_near, [(block, F32), (block, BF16)] * 2, keep.reshape(shape), swap(send.reshape(shape), 1)
    )
    block = (far, half, width)
    first, first_out, second, second_out = add(
        add_next,
        [(block, F32), (block, BF16)] * 2,
        first,
        swap(first_out, 2),
        second,
        swap(second_out, 4),
    )
    block = (tiles, width)
    sums, *parts = add(
        add_far,
        [(block, F32)] + [(block, BF16)] * (far - 1),
        first,
        swap(first_out, 4),
        second,
        swap(second_out, 2),
    )
    here = []
    for s, part in zip(range(1, far), parts):
        here.append(swap(part, s << 3))
    parts = here
    for part in parts:
        sums = sums + part.astype(F32)
    part = guest_rows // 2
    wide = pl.BlockSpec((part, width), lambda i: (i, 0))
    new_state, counts = pl.pallas_call(
        finish_kernel,
        out_shape=(
            jax.ShapeDtypeStruct((capacity, width), F32),
            jax.ShapeDtypeStruct((tiles, width), F32),
        ),
        grid=(-(-capacity // part),),
        in_specs=[SMEM] * 2
        + [
            wide,
            wide,
            pl.BlockSpec((part, width), lambda i: (jnp.minimum(i, 1), 0)),
            pl.BlockSpec((1, columns), lambda i: (0, 0)),
        ],
        out_specs=(wide, pl.BlockSpec((tiles, width), lambda i: (0, 0))),
        cost_estimate=cost(4.0),
        compiler_params=small,
        name="finish",
    )(owner_counts, other_count, land_state, tend, back, column_tile.reshape(1, columns))
    tile_flux = sums / jnp.maximum(counts, 1.0)
    return (new_state, tile_flux)


def solution(mesh):
    devices = mesh.shape["atm"] * mesh.shape["land"]
    rows, whole = P(AXES, None), P()

    def body(*arrays):
        return local(devices, *arrays)

    return jax.shard_map(
        body,
        mesh=mesh,
        in_specs=(rows, P(AXES), whole, P(AXES), P(AXES), P(AXES), rows) + (whole,) * 5,
        out_specs=(rows, rows),
        check_vma=False,
    )
```
